32 devices in a mesh: gx: 4 (over y, x), gy: 4 (over z), gz: 2 (over core).
Axes of the slice: x: 2, y: 2, z: 4, core: 2. Of those that a mesh axis runs over, the one named last changes fastest.
Arguments:
- positions: float32 [12, 12, 16, 96], P('gx', 'gy', 'gz'), may hold values from 0 to 1
- types: int32 [12, 12, 16, 32], P('gx', 'gy', 'gz'), may hold values from 0 to 2
Outputs:
- forces_energy: float32 [12, 12, 16, 128], P('gx', 'gy', 'gz')
The draws below stay inside these ranges and needn't reach their ends.
Inputs may be any that keep to these rules, and one draw needn't show every extreme that they name: `types`: 0 marks an empty slot, 1 a copper atom, 2 a nickel atom.
All inputs are finite; a program needn't handle non-finite values.
Results may differ from the reference program's by a relative error of at most 0.0001.
Values sent between devices are 32-bit elements; how exact they have to be, the bound alone decides.
A program may use at most 64 MiB of HBM per device.

```python
import jax
import jax.numpy as jnp
from jax import lax

S = 32
NX = 12
NY = 12
NZ = 16


def set_ends(entries, key, least, top_value):
    index_at = [jax.random.randint(jax.random.fold_in(key, axis), (), 0, length) for axis, length in enumerate(entries.shape)]
    main_axis = entries.shape.index(max(entries.shape))
    beside = index_at[:main_axis] + [(index_at[main_axis] + 1) % entries.shape[main_axis]] + index_at[main_axis + 1:]
    return entries.at[tuple(index_at)].set(least).at[tuple(beside)].set(top_value)


def shard_levels(stream_key, dims, cuts, smallest, largest):
    level, own = 1.0, jax.random.fold_in(stream_key, 6)
    for axis_at, shards_of in cuts:
        draws = jnp.exp(jax.random.uniform(jax.random.fold_in(own, axis_at), (shards_of,), jnp.float32, smallest / len(cuts), largest / len(cuts)))
        level = level * jnp.repeat(draws, dims[axis_at] // shards_of).reshape([-1 if axis == axis_at else 1 for axis in range(len(dims))])
    return level


def setup_inputs(seed: int = 0) -> dict:
    key_list = jax.random.split(jax.random.key(seed), 3)
    return {
        "positions": jnp.clip(1.0 * jax.random.uniform(key_list[0], (NX, NY, NZ, 3 * S), jnp.float32) ** shard_levels(key_list[0], (NX, NY, NZ, 3 * S), ((0, 4), (1, 4), (2, 2)), -0.2, 0.2), 0.0, 1.0),
        "types": set_ends(jax.random.randint(key_list[1], (NX, NY, NZ, S), 0, 3), jax.random.fold_in(key_list[1], 1), 0, 2).astype(jnp.int32),
    }


cut_square = 0.9025
density_rate = 3.0
pair_rate = 6.0

def type_tables(types):
    weight = jnp.where(types == 1, 1.0, jnp.where(types == 2, 1.6, 0.0)).astype(jnp.float32)
    embedding = jnp.where(types == 1, 1.0, jnp.where(types == 2, 1.4, 0.0)).astype(jnp.float32)
    return (weight, embedding)

def separation(own_coords, other_coords, cell_shift):
    shift_vector = jnp.asarray(cell_shift, jnp.float32).reshape(3, 1, 1)
    displace = shift_vector + other_coords[..., :, None, :] - own_coords[..., :, :, None]
    return (displace, lax.optimization_barrier(jnp.sum(displace * displace, axis=-3)))

def density_shape(square):
    margin = jnp.maximum(1.0 - square / cut_square, 0.0)
    return jnp.exp(-density_rate * square) * margin * margin

def all_shapes(square):
    margin = jnp.maximum(1.0 - square / cut_square, 0.0)
    density_exponent = jnp.exp(-density_rate * square)
    pair_exp = jnp.exp(-pair_rate * square)
    dens_slope = -density_exponent * margin * (density_rate * margin + 2.0 / cut_square)
    pair_value = pair_exp * margin * margin
    pair_slope = -pair_exp * margin * (pair_rate * margin + 2.0 / cut_square)
    return (dens_slope, pair_value, pair_slope)

def neighbour_shifts():
    return [(a, b, c) for a in (-1, 0, 1) for b in (-1, 0, 1) for c in (-1, 0, 1)]

def reference(positions, types):
    size_x, size_y, size_z, slots = types.shape
    coords = positions.reshape(size_x, size_y, size_z, 3, slots)
    weight, embedding = type_tables(types)
    margins = ((1, 1), (1, 1), (1, 1), (0, 0))
    pad_coords = jnp.pad(coords, margins + ((0, 0),), mode='wrap')
    pad_weight = jnp.pad(weight, margins, mode='wrap')
    distinct = 1.0 - jnp.eye(slots, dtype=jnp.float32)
    plane_ids = jnp.arange(size_x).astype(jnp.int32)

    def neighbour(padded, plane_index, cell_shift):
        x_layer = lax.dynamic_index_in_dim(padded, plane_index + 1 + cell_shift[0], 0, keepdims=False)
        return x_layer[1 + cell_shift[1]:1 + cell_shift[1] + size_y, 1 + cell_shift[2]:1 + cell_shift[2] + size_z]

    def own_plane(array, plane_index):
        return lax.dynamic_index_in_dim(array, plane_index, 0, keepdims=False)

    def density_plane(plane_index):
        own_coords = own_plane(coords, plane_index)
        summed = jnp.zeros((size_y, size_z, slots), jnp.float32)
        for cell_shift in neighbour_shifts():
            other_coords = neighbour(pad_coords, plane_index, cell_shift)
            other_weight = neighbour(pad_weight, plane_index, cell_shift)
            displace, square = separation(own_coords, other_coords, cell_shift)
            dens = density_shape(square)
            if cell_shift == (0, 0, 0):
                dens = dens * distinct
            summed = summed + lax.optimization_barrier(jnp.sum(dens * other_weight[..., None, :], axis=-1))
        return summed
    density_sum = lax.map(density_plane, plane_ids)
    root_value = jnp.sqrt(density_sum + 1.0)
    slope = -embedding / (2.0 * root_value)
    pad_slope = jnp.pad(slope, margins, mode='wrap')

    def force_plane(plane_index):
        own_coords = own_plane(coords, plane_index)
        own_weight = own_plane(weight, plane_index)
        own_slope = own_plane(slope, plane_index)
        force_sum = jnp.zeros((size_y, size_z, 3, slots), jnp.float32)
        pair_sum = jnp.zeros((size_y, size_z, slots), jnp.float32)
        for cell_shift in neighbour_shifts():
            other_coords = neighbour(pad_coords, plane_index, cell_shift)
            other_weight = neighbour(pad_weight, plane_index, cell_shift)
            other_slope = neighbour(pad_slope, plane_index, cell_shift)
            displace, square = separation(own_coords, other_coords, cell_shift)
            dens_slope, pair_value, pair_slope = all_shapes(square)
            both_weight = own_weight[..., :, None] * other_weight[..., None, :]
            coupling = (own_slope[..., :, None] * other_weight[..., None, :] + other_slope[..., None, :] * own_weight[..., :, None]) * dens_slope + 0.5 * both_weight * pair_slope
            energy_pair = 0.25 * both_weight * pair_value
            if cell_shift == (0, 0, 0):
                coupling = coupling * distinct
                energy_pair = energy_pair * distinct
            force_sum = force_sum + 2.0 * lax.optimization_barrier(jnp.sum(coupling[..., None, :, :] * displace, axis=-1))
            pair_sum = pair_sum + lax.optimization_barrier(jnp.sum(energy_pair, axis=-1))
        return (force_sum, pair_sum)
    force_all, pair_all = lax.map(force_plane, plane_ids)
    energy_all = pair_all - embedding * root_value
    return jnp.concatenate([force_all.reshape(size_x, size_y, size_z, 3 * slots), energy_all], axis=-1)
```

```python
import functools
import math

import jax
import jax.numpy as jnp
from jax import lax
from jax.experimental import pallas as pl
from jax.experimental.pallas import tpu as pltpu
from jax.sharding import PartitionSpec as P

cut_square = 0.9025
density_rate = 3.0
unit = density_rate * math.log2(math.e)
alpha = math.sqrt(unit)
kappa = unit * cut_square
tail = 2.0**-kappa
shift_big = 2.0 * kappa / (cut_square * density_rate)
density_scale = tail / kappa**2
energy_scale = 0.25 * tail**2 / kappa**2
force_scale = -2.0 * tail**2 * density_rate / (kappa**2 * alpha)
slope_scale = -0.5 / tail

AXES = ("gx", "gy", "gz")
DIRECTIONS = sorted(
    (
        (a, b, c)
        for a in (-1, 0, 1)
        for b in (-1, 0, 1)
        for c in (-1, 0, 1)
        if (a, b, c) != (0, 0, 0)
    ),
    key=lambda d: -(2 * abs(d[0]) + 2 * abs(d[1]) + abs(d[2])),
)
WIDE = 128


def kernel(dims, axis_sizes, pos_ref, typ_ref, out_ref, pos, typ, pad, pad_phi, spread, spread_phi,
           own, acc, acc_force, rows, phi_rows, hot, pair_e, pair_m, pair_q,
           load_sem, send_sem, recv_sem, send_phi, recv_phi):
    nx, ny, nz, slots = dims
    lanes = nz * slots
    base = 8
    me = [lax.axis_index(axis) for axis in AXES]

    def peer(direction):
        return {
            axis: lax.rem(place + step + size, size)
            for axis, place, step, size in zip(AXES, me, direction, axis_sizes)
        }

    barrier = pltpu.get_barrier_semaphore()
    for direction in DIRECTIONS:
        pl.semaphore_signal(
            barrier, inc=1, device_id=peer(direction), device_id_type=pl.DeviceIdType.MESH
        )
    loads = [
        pltpu.make_async_copy(pos_ref, pos, load_sem.at[0]),
        pltpu.make_async_copy(typ_ref, typ, load_sem.at[1]),
    ]
    for load in loads:
        load.start()

    row = lax.broadcasted_iota(jnp.int32, (3 * nz, lanes), 0) % nz
    cell = lax.broadcasted_iota(jnp.int32, (3 * nz, lanes), 1) // slots
    hot[...] = jnp.where(row == cell, 1.0, 0.0).astype(jnp.bfloat16)
    diagonal = (
        lax.broadcasted_iota(jnp.int32, (slots, lanes), 1) % slots
        == lax.broadcasted_iota(jnp.int32, (slots, lanes), 0)
    )
    cell_mask = (
        lax.broadcasted_iota(jnp.int32, (nz, lanes), 1) // slots
        == lax.broadcasted_iota(jnp.int32, (nz, lanes), 0)
    )
    group = lax.broadcasted_iota(jnp.int32, (nz, WIDE), 1) // slots

    for load in loads:
        load.wait()
    for x in range(nx):
        for y in range(ny):
            kind = typ[x, y]
            weight = jnp.where(kind == 1, 1.0, jnp.where(kind == 2, 1.6, 0.0)).astype(jnp.float32)
            pad[x + 1, y + 1, base : base + nz, :] = jnp.concatenate(
                [pos[x, y] * alpha, weight], axis=1
            )

    def pieces(value):
        high = value.astype(jnp.bfloat16).astype(jnp.float32)
        rest = value - high
        middle = rest.astype(jnp.bfloat16).astype(jnp.float32)
        return high, middle, rest - middle

    def spread_out(blocks):
        wide = blocks[0] if len(blocks) == 1 else jnp.concatenate(blocks, axis=1)
        stacked = jnp.concatenate(pieces(wide), axis=0).astype(jnp.bfloat16)
        return lax.dot_general(
            stacked, hot[...], (((0,), (0,)), ((), ())), preferred_element_type=jnp.float32
        )

    def expand(blocks):
        result = spread_out(
            [pad[x, y, base - 1 + dz : base - 1 + dz + nz, :] for x, y, dz in blocks]
        )
        for k, (x, y, dz) in enumerate(blocks):
            spread[x, y, dz] = result[k * WIDE : (k + 1) * WIDE]

    many = WIDE // slots

    def expand_phi(blocks):
        wide = []
        for start in range(0, len(blocks), many):
            part = [
                pad_phi[x, y, base - 1 + dz : base - 1 + dz + nz, :]
                for x, y, dz in blocks[start : start + many]
            ]
            value = part[-1]
            for k in reversed(range(len(part) - 1)):
                value = jnp.where(group == k, part[k], value)
            wide.append(value)
        result = spread_out(wide)
        for k, (x, y, dz) in enumerate(blocks):
            spread_phi[x, y, dz] = result[k * slots : (k + 1) * slots]

    def density(x, y, a, b, layers, sums):
        rho, energy = sums
        t, n = x * ny + y, 3 * a + b
        px = own[t, 0:1, :] - jnp.asarray(a - 1, jnp.float32) * alpha
        py = own[t, 1:2, :] - jnp.asarray(b - 1, jnp.float32) * alpha
        px = jnp.broadcast_to(px, (8, lanes))
        py = jnp.broadcast_to(py, (8, lanes))
        for dz in layers:
            pz = jnp.broadcast_to(own[t, 2:3, :] - (dz - 1) * alpha, (8, lanes))
            for r in range(0, slots, 8):
                dx = spread[x + a, y + b, dz, r : r + 8, :] - px
                dy = spread[x + a, y + b, dz, slots + r : slots + r + 8, :] - py
                dd = spread[x + a, y + b, dz, 2 * slots + r : 2 * slots + r + 8, :] - pz
                wj = spread[x + a, y + b, dz, 3 * slots + r : 3 * slots + r + 8, :]
                m = jnp.maximum(kappa - (dx * dx + dy * dy + dd * dd), 0.0)
                e = jnp.exp2(m)
                em = e * m
                q = em * wj
                rho = rho + q * m
                energy = energy + q * em
                pair_e[t, n, dz, r : r + 8, :] = e
                pair_m[t, n, dz, r : r + 8, :] = m
                pair_q[t, n, dz, r : r + 8, :] = q
        return rho, energy

    def force(x, y, a, b, layers, sums):
        fx, fy, fz = sums
        t, n = x * ny + y, 3 * a + b
        px = own[t, 0:1, :] - jnp.asarray(a - 1, jnp.float32) * alpha
        py = own[t, 1:2, :] - jnp.asarray(b - 1, jnp.float32) * alpha
        px = jnp.broadcast_to(px, (8, lanes))
        py = jnp.broadcast_to(py, (8, lanes))
        phi = jnp.broadcast_to(own[t, 4:5, :], (8, lanes))
        for dz in layers:
            pz = jnp.broadcast_to(own[t, 2:3, :] - (dz - 1) * alpha, (8, lanes))
            for r in range(0, slots, 8):
                dx = spread[x + a, y + b, dz, r : r + 8, :] - px
                dy = spread[x + a, y + b, dz, slots + r : slots + r + 8, :] - py
                dd = spread[x + a, y + b, dz, 2 * slots + r : 2 * slots + r + 8, :] - pz
                e = pair_e[t, n, dz, r : r + 8, :]
                m = pair_m[t, n, dz, r : r + 8, :]
                q = pair_q[t, n, dz, r : r + 8, :]
                both = phi + spread_phi[x + a, y + b, dz, r : r + 8, :]
                v = q * (both * (m + shift_big) + e * (m + 0.5 * shift_big))
                fx = fx + v * dx
                fy = fy + v * dy
                fz = fz + v * dd
        return fx, fy, fz

    def over(function, target, x, y, a_range, b_range, layers, fresh):
        t = x * ny + y
        count = target.shape[1]
        zero = jnp.zeros((8, lanes), jnp.float32)
        sums = tuple(zero if fresh else target[t, k] for k in range(count))

        def along(a, sums):
            return lax.fori_loop(
                b_range[0], b_range[1], lambda b, s: function(x, y, a, b, layers, s), sums
            )

        if isinstance(a_range, int):
            sums = along(a_range, sums)
        else:
            sums = lax.fori_loop(a_range[0], a_range[1], along, sums)
        for k in range(count):
            target[t, k] = sums[k]

    def inside(place, length):
        return jnp.maximum(0, 1 - place), jnp.minimum(3, length + 1 - place)

    def own_pairs(function, target, layers, fresh):
        def column(t, carry):
            x, y = t // ny, t % ny
            over(function, target, x, y, inside(x, nx), inside(y, ny), layers, fresh)
            return carry

        lax.fori_loop(0, nx * ny, column, 0)

    def side_pairs(function, target, a, b):
        every = (0, 1, 2)
        edge = {-1: 0, 1: None}
        if a and b:
            x, y = (0 if a < 0 else nx - 1), (0 if b < 0 else ny - 1)
            over(function, target, x, y, a + 1, (b + 1, b + 2), every, False)
        elif a:
            x = 0 if a < 0 else nx - 1

            def along_y(y, carry):
                over(function, target, x, y, a + 1, inside(y, ny), every, False)
                return carry

            lax.fori_loop(0, ny, along_y, 0)
        else:
            y = 0 if b < 0 else ny - 1

            def along_x(x, carry):
                over(function, target, x, y, inside(x, nx), (b + 1, b + 2), every, False)
                return carry

            lax.fori_loop(0, nx, along_x, 0)

    def halo_columns(a, b):
        xs = range(1, nx + 1) if a == 0 else [0 if a < 0 else nx + 1]
        ys = range(1, ny + 1) if b == 0 else [0 if b < 0 else ny + 1]
        return [(x, y) for x in xs for y in ys]

    own_columns = halo_columns(0, 0)
    sides = [(-1, 0), (1, 0), (0, -1), (0, 1), (-1, -1), (-1, 1), (1, -1), (1, 1)]

    def start_exchange(buffer, send, recv):
        def source(step, length):
            return (
                pl.ds(length, 1) if step > 0 else pl.ds(1, 1) if step < 0 else pl.ds(1, length)
            )

        def target(step, length):
            return (
                pl.ds(0, 1)
                if step > 0
                else pl.ds(length + 1, 1) if step < 0 else pl.ds(1, length)
            )

        def source_z(step):
            return (
                pl.ds(base + nz - 1, 1)
                if step > 0
                else pl.ds(base, 1) if step < 0 else pl.ds(base, nz)
            )

        def target_z(step):
            return (
                pl.ds(base - 1, 1)
                if step > 0
                else pl.ds(base + nz, 1) if step < 0 else pl.ds(base, nz)
            )

        copies = {}
        for index, direction in enumerate(DIRECTIONS):
            a, b, c = direction
            copy = pltpu.make_async_remote_copy(
                src_ref=buffer.at[source(a, nx), source(b, ny), source_z(c)],
                dst_ref=buffer.at[target(a, nx), target(b, ny), target_z(c)],
                send_sem=send.at[index],
                recv_sem=recv.at[index],
                device_id=peer(direction),
                device_id_type=pl.DeviceIdType.MESH,
            )
            copy.start()
            copies[direction] = copy
        return copies

    def arrive(copies, a, b):
        for c in (0, -1, 1):
            if (a, b, c) != (0, 0, 0):
                copies[(-a, -b, -c)].wait_recv()

    expand([(x, y, 1) for x, y in own_columns])
    for x in range(nx):
        for y in range(ny):
            for k in range(4):
                own[x * ny + y, k : k + 1, :] = jnp.sum(
                    jnp.where(
                        diagonal, spread[x + 1, y + 1, 1, k * slots : (k + 1) * slots, :], 0.0
                    ),
                    axis=0,
                    keepdims=True,
                )
    own_pairs(density, acc, (1,), True)

    pl.semaphore_wait(barrier, len(DIRECTIONS))
    copies = start_exchange(pad, send_sem, recv_sem)
    arrive(copies, 0, 0)
    for x in range(1, nx + 1):
        expand([(x, y, dz) for y in range(1, ny + 1) for dz in (0, 2)])
    own_pairs(density, acc, (0, 2), False)
    for a, b in sides:
        arrive(copies, a, b)
        expand([(x, y, dz) for x, y in halo_columns(a, b) for dz in range(3)])
        side_pairs(density, acc, a, b)

    for t in range(nx * ny):
        for k in range(2):
            rows[k, t : t + 1, :] = jnp.sum(acc[t, k], axis=0, keepdims=True)
        rows[2, t : t + 1, :] = own[t, 3:4, :]
    w = rows[2]
    rho = rows[0] * density_scale - w
    root = jnp.sqrt(jnp.maximum(rho, 0.0) + 1.0)
    big = w > 1.3
    ratio = jnp.where(big, 0.875, jnp.where(w > 0.5, 1.0, 0.0))
    phi_rows[...] = slope_scale * ratio / root
    rows[3] = root

    def fold(line):
        value = jnp.where(cell_mask, jnp.broadcast_to(line, (nz, lanes)), 0.0)
        total = value[:, :WIDE]
        for start in range(WIDE, lanes, WIDE):
            total = total + value[:, start : start + WIDE]
        step = WIDE // 2
        while step >= slots:
            total = total + pltpu.roll(total, step, 1)
            step //= 2
        return total

    for x in range(nx):
        for y in range(ny):
            t = x * ny + y
            line = phi_rows[t : t + 1, :]
            own[t, 4:5, :] = line
            pad_phi[x + 1, y + 1, base : base + nz, :] = fold(line)

    copies_phi = start_exchange(pad_phi, send_phi, recv_phi)

    energy = rows[1] * (energy_scale * w) - 0.25 * w * w
    a_coef = jnp.where(big, 1.4, jnp.where(w > 0.5, 1.0, 0.0))
    rows[3] = energy - a_coef * rows[3]

    expand_phi([(x, y, 1) for x, y in own_columns])
    own_pairs(force, acc_force, (1,), True)
    arrive(copies_phi, 0, 0)
    expand_phi([(x, y, dz) for x, y in own_columns for dz in (0, 2)])
    own_pairs(force, acc_force, (0, 2), False)
    for a, b in sides:
        arrive(copies_phi, a, b)
        expand_phi([(x, y, dz) for x, y in halo_columns(a, b) for dz in range(3)])
        side_pairs(force, acc_force, a, b)

    for x in range(nx):
        for y in range(ny):
            t = x * ny + y
            scale = force_scale * own[t, 3:4, :]
            lines = [
                fold(jnp.sum(acc_force[t, k], axis=0, keepdims=True) * scale) for k in range(3)
            ] + [fold(rows[3, t : t + 1, :])]
            value = lines[3]
            for k in range(3):
                value = jnp.where(group == k, lines[k], value)
            out_ref[x, y] = value

    for direction in DIRECTIONS:
        copies[direction].wait_send()
        copies_phi[direction].wait_send()


def body(axis_sizes, positions, types):
    nx, ny, nz, slots = types.shape
    lanes = nz * slots
    count = len(DIRECTIONS)
    columns = nx * ny
    deep = 16 + nz
    return pl.pallas_call(
        functools.partial(kernel, (nx, ny, nz, slots), axis_sizes),
        out_shape=jax.ShapeDtypeStruct((nx, ny, nz, 4 * slots), jnp.float32),
        in_specs=[pl.BlockSpec(memory_space=pl.ANY), pl.BlockSpec(memory_space=pl.ANY)],
        out_specs=pl.BlockSpec(memory_space=pltpu.VMEM),
        scratch_shapes=[
            pltpu.VMEM((nx, ny, nz, 3 * slots), jnp.float32),
            pltpu.VMEM((nx, ny, nz, slots), jnp.int32),
            pltpu.VMEM((nx + 2, ny + 2, deep, WIDE), jnp.float32),
            pltpu.VMEM((nx + 2, ny + 2, deep, WIDE), jnp.float32),
            pltpu.VMEM((nx + 2, ny + 2, 3, 4 * slots, lanes), jnp.float32),
            pltpu.VMEM((nx + 2, ny + 2, 3, slots, lanes), jnp.float32),
            pltpu.VMEM((columns, 8, lanes), jnp.float32),
            pltpu.VMEM((columns, 2, 8, lanes), jnp.float32),
            pltpu.VMEM((columns, 3, 8, lanes), jnp.float32),
            pltpu.VMEM((4, columns, lanes), jnp.float32),
            pltpu.VMEM((columns, lanes), jnp.float32),
            pltpu.VMEM((3 * nz, lanes), jnp.bfloat16),
            pltpu.VMEM((columns, 9, 3, slots, lanes), jnp.float32),
            pltpu.VMEM((columns, 9, 3, slots, lanes), jnp.float32),
            pltpu.VMEM((columns, 9, 3, slots, lanes), jnp.float32),
            pltpu.SemaphoreType.DMA((2,)),
            pltpu.SemaphoreType.DMA((count,)),
            pltpu.SemaphoreType.DMA((count,)),
            pltpu.SemaphoreType.DMA((count,)),
            pltpu.SemaphoreType.DMA((count,)),
        ],
        compiler_params=pltpu.CompilerParams(
            collective_id=0, has_side_effects=True, vmem_limit_bytes=60 * 1024 * 1024
        ),
    )(positions, types)


def solution(mesh):
    spec = P("gx", "gy", "gz", None)
    sizes = tuple(mesh.shape[axis] for axis in AXES)
    return jax.shard_map(
        functools.partial(body, sizes),
        mesh=mesh,
        in_specs=(spec, spec),
        out_specs=spec,
        check_vma=False,
    )
```

```python
import functools
import math

import jax
import jax.numpy as jnp
from jax import lax
from jax.experimental import pallas as pl
from jax.experimental.pallas import tpu as pltpu
from jax.sharding import PartitionSpec as P

cut_square = 0.9025
density_rate = 3.0
unit = density_rate * math.log2(math.e)
alpha = math.sqrt(unit)
kappa = unit * cut_square
tail = 2.0**-kappa
shift_big = 2.0 * kappa / (cut_square * density_rate)
density_scale = tail / kappa**2
energy_scale = 0.25 * tail**2 / kappa**2
force_scale = -2.0 * tail**2 * density_rate / (kappa**2 * alpha)
slope_scale = -0.5 / tail
far = 1.0e4

AXES = ("gx", "gy", "gz")
DIRECTIONS = sorted(
    (
        (a, b, c)
        for a in (-1, 0, 1)
        for b in (-1, 0, 1)
        for c in (-1, 0, 1)
        if (a, b, c) != (0, 0, 0)
    ),
    key=lambda d: -(2 * abs(d[0]) + 2 * abs(d[1]) + abs(d[2])),
)
SIDES = [(-1, 0), (1, 0), (0, -1), (0, 1), (-1, -1), (-1, 1), (1, -1), (1, 1)]
WIDE = 128
DEEP = 256


def kernel(dims, axis_sizes, pos_ref, typ_ref, out_ref, pos, typ, pad, pad_phi, left, right, moment,
           spread_w, spread_phi, own, acc, acc_force, rows, phi_rows, hot, pair_m, pair_e,
           load_sem, send_sem, recv_sem, send_phi, recv_phi):
    nx, ny, nz, slots = dims
    lanes = nz * slots
    tall = 3 * slots
    base = 8
    f32, bf16 = jnp.float32, jnp.bfloat16
    me = [lax.axis_index(axis) for axis in AXES]

    def peer(direction):
        return {
            axis: lax.rem(place + step + size, size)
            for axis, place, step, size in zip(AXES, me, direction, axis_sizes)
        }

    barrier = pltpu.get_barrier_semaphore()
    for direction in DIRECTIONS:
        pl.semaphore_signal(
            barrier, inc=1, device_id=peer(direction), device_id_type=pl.DeviceIdType.MESH
        )
    loads = [
        pltpu.make_async_copy(pos_ref, pos, load_sem.at[0]),
        pltpu.make_async_copy(typ_ref, typ, load_sem.at[1]),
    ]
    for load in loads:
        load.start()

    cell_mask = (
        lax.broadcasted_iota(jnp.int32, (nz, lanes), 1) // slots
        == lax.broadcasted_iota(jnp.int32, (nz, lanes), 0)
    )
    cells = jnp.where(cell_mask, 1.0, 0.0).astype(f32)
    group = lax.broadcasted_iota(jnp.int32, (nz, WIDE), 1) // slots
    empty = jnp.zeros((nz, lanes), f32)
    full = jnp.ones((nz, WIDE), f32)
    none = jnp.zeros((nz, WIDE), f32)
    parts = DEEP // nz
    used = 27
    hot[...] = jnp.concatenate(
        [empty] * (used - 3) + [cells] * 3 + [empty] * (parts - used), axis=0
    ).astype(bf16)

    for load in loads:
        load.wait()
    for x in range(nx):
        for y in range(ny):
            kind = typ[x, y]
            weight = jnp.where(kind == 1, 1.0, jnp.where(kind == 2, 1.6, 0.0)).astype(f32)
            pad[x + 1, y + 1, base : base + nz, :] = jnp.concatenate(
                [pos[x, y] * alpha, weight], axis=1
            )

    def pieces(value):
        high = value.astype(bf16).astype(f32)
        rest = value - high
        middle = rest.astype(bf16).astype(f32)
        return high, middle, rest - middle

    def choose(values):
        result = values[-1]
        for k in reversed(range(len(values) - 1)):
            result = jnp.where(group == k, values[k], result)
        return result

    def turn(value, step):
        step = (step * slots) % WIDE
        return pltpu.roll(value, step, 1) if step else value

    def centre(k, place):
        return (place - 0.5 * ((nx, ny)[k] + 1) - 0.5) * alpha

    layer = (group.astype(f32) - 1.5) * alpha

    def neighbour(x, y):
        shifted = [pad[x, y, base - 1 + dz : base - 1 + dz + nz, :] for dz in range(3)]
        px, py, pz, w = (
            choose([turn(shifted[dz], dz - q) for dz in range(3)]) for q in range(4)
        )
        px = px + centre(0, x)
        py = py + centre(1, y)
        pz = pz + layer
        square = px * px + py * py + pz * pz
        square = jnp.where(w > 0.0, square, far)
        lines = []
        for value in (px, py, pz):
            h, m, l = pieces(value)
            lines += [h, m, h, l, m, h]
        lines += list(pieces(-square)) + [full] * 3
        ws = list(pieces(w))
        lines += ws + [none] * (parts - used)
        stacked = jnp.concatenate(lines, axis=0).astype(bf16)
        left[x, y] = stacked.T[:tall]
        terms = []
        for value in (w * px, w * py, w * pz):
            terms += list(pieces(value))
        terms = jnp.concatenate(terms + ws, axis=0)
        turned = pltpu.roll(terms, tall, 1)
        lane = lax.broadcasted_iota(jnp.int32, terms.shape, 1)
        moment[x, y, :, :WIDE] = jnp.where(lane < tall, terms, turned).astype(bf16)
        moment[x, y, :, WIDE:] = jnp.where(lane < 2 * tall - WIDE, turned, 0.0).astype(bf16)

    def spread_weight(x, y):
        spread_w[x, y] = jnp.dot(left[x, y], hot[...], preferred_element_type=f32)

    def owner(x, y):
        t = (x - 1) * ny + y - 1
        value = pad[x, y, base : base + nz, :]
        px, py, pz, w = (choose([turn(value, g - q) for g in range(WIDE // slots)]) for q in range(4))
        px = px + centre(0, x)
        py = py + centre(1, y)
        pz = pz - 0.5 * alpha
        square = kappa - (px * px + py * py + pz * pz)

        def tile(value):
            return jnp.where(cell_mask, jnp.concatenate([value] * (lanes // WIDE), axis=1), 0.0)

        lines = []
        for value in (px, py, pz):
            h, m, l = (tile(2.0 * piece) for piece in pieces(value))
            lines += [h, h, m, h, m, l]
        lines += [cells] * 3 + [tile(piece) for piece in pieces(square)]
        lines += [empty] * (parts - used + 3)
        right[t] = jnp.concatenate(lines, axis=0).astype(bf16)
        for k, value in enumerate((px, py, pz, w)):
            own[t, k] = tile(value)
        rows[2, t : t + 1, :] = jnp.sum(own[t, 3], axis=0, keepdims=True)

    def pair(x, y, a, b):
        return (((x - 1) * ny + y - 1) * 3 + a) * 3 + b

    def density(x, y, offsets, fresh):
        t = (x - 1) * ny + y - 1
        zero = jnp.zeros((8, lanes), f32)
        rho, energy = (zero, zero) if fresh else (acc[t, 0], acc[t, 1])
        for a, b in offsets:
            n = pair(x, y, a, b)
            column = (x + a - 1, y + b - 1)
            margin = jnp.dot(left[column], right[t], preferred_element_type=f32)
            for r in range(0, tall, 8):
                m = jnp.maximum(margin[r : r + 8], 0.0)
                e = jnp.exp2(m)
                u = e * m
                q = u * spread_w[column[0], column[1], r : r + 8, :]
                rho = rho + q * m
                energy = energy + q * u
                pair_m[n, r : r + 8, :] = m
                pair_e[n, r : r + 8, :] = e
        acc[t, 0] = rho
        acc[t, 1] = energy

    def slopes(n, carry):
        for r in range(0, tall, 8):
            m = pair_m[n, r : r + 8, :]
            e = pair_e[n, r : r + 8, :]
            u = e * m
            pair_m[n, r : r + 8, :] = u * (m + shift_big)
            pair_e[n, r : r + 8, :] = u * (e * (m + 0.5 * shift_big))
        return carry

    def force(x, y, offsets, fresh):
        t = (x - 1) * ny + y - 1
        phi = jnp.broadcast_to(phi_rows[t : t + 1, :], (slots, lanes))
        total = None
        for a, b in offsets:
            n = pair(x, y, a, b)
            column = (x + a - 1, y + b - 1)
            high, low = [], []
            for r in range(0, tall, slots):
                both = phi + spread_phi[column[0], column[1], r : r + slots, :]
                v = both * pair_m[n, r : r + slots, :] + pair_e[n, r : r + slots, :]
                top = v.astype(bf16)
                high.append(top)
                low.append((v - top.astype(f32)).astype(bf16))
            values = jnp.concatenate(high + low, axis=0)
            part = jnp.dot(
                moment[column[0], column[1], :, : 2 * tall], values, preferred_element_type=f32
            )
            total = part if total is None else total + part
        acc_force[t] = total if fresh else acc_force[t] + total

    def halo_columns(a, b):
        xs = range(1, nx + 1) if a == 0 else [0 if a < 0 else nx + 1]
        ys = range(1, ny + 1) if b == 0 else [0 if b < 0 else ny + 1]
        return [(x, y) for x in xs for y in ys]

    own_columns = halo_columns(0, 0)

    def work(function, columns, fresh):
        for x, y in own_columns:
            offsets = [
                (a, b)
                for a in range(3)
                for b in range(3)
                if (x + a - 1, y + b - 1) in columns
            ]
            if offsets:
                function(x, y, offsets, fresh)

    many = WIDE // slots

    def expand_phi(columns):
        wide = [
            choose(
                [pad_phi[x, y, base - 1 + dz : base - 1 + dz + nz, :] for dz in range(3)]
            )
            for x, y in columns
        ]
        wide = wide[0] if len(wide) == 1 else jnp.concatenate(wide, axis=1)
        stacked = jnp.concatenate(pieces(wide), axis=0).astype(bf16)
        result = lax.dot_general(
            stacked,
            hot[(used - 3) * nz : used * nz, :],
            (((0,), (0,)), ((), ())),
            preferred_element_type=f32,
        )
        for k, (x, y) in enumerate(columns):
            spread_phi[x, y] = result[k * WIDE : k * WIDE + tall]

    def start_exchange(buffer, send, recv):
        def source(step, length):
            return (
                pl.ds(length, 1) if step > 0 else pl.ds(1, 1) if step < 0 else pl.ds(1, length)
            )

        def target(step, length):
            return (
                pl.ds(0, 1)
                if step > 0
                else pl.ds(length + 1, 1) if step < 0 else pl.ds(1, length)
            )

        def source_z(step):
            return (
                pl.ds(base + nz - 1, 1)
                if step > 0
                else pl.ds(base, 1) if step < 0 else pl.ds(base, nz)
            )

        def target_z(step):
            return (
                pl.ds(base - 1, 1)
                if step > 0
                else pl.ds(base + nz, 1) if step < 0 else pl.ds(base, nz)
            )

        copies = {}
        for index, direction in enumerate(DIRECTIONS):
            a, b, c = direction
            copy = pltpu.make_async_remote_copy(
                src_ref=buffer.at[source(a, nx), source(b, ny), source_z(c)],
                dst_ref=buffer.at[target(a, nx), target(b, ny), target_z(c)],
                send_sem=send.at[index],
                recv_sem=recv.at[index],
                device_id=peer(direction),
                device_id_type=pl.DeviceIdType.MESH,
            )
            copy.start()
            copies[direction] = copy
        return copies

    def arrive(copies, a, b):
        for c in (0, -1, 1):
            if (a, b, c) != (0, 0, 0):
                copies[(-a, -b, -c)].wait_recv()

    for x, y in own_columns:
        owner(x, y)

    pl.semaphore_wait(barrier, len(DIRECTIONS))
    copies = start_exchange(pad, send_sem, recv_sem)
    arrive(copies, 0, 0)
    for columns in [own_columns] + SIDES:
        if columns is not own_columns:
            arrive(copies, *columns)
            columns = halo_columns(*columns)
        for x, y in columns:
            neighbour(x, y)
        for x, y in columns:
            spread_weight(x, y)
        work(density, columns, columns is own_columns)

    for t in range(nx * ny):
        for k in range(2):
            rows[k, t : t + 1, :] = jnp.sum(acc[t, k], axis=0, keepdims=True)
    w = rows[2]
    rho = rows[0] * density_scale - w
    root = jnp.sqrt(jnp.maximum(rho, 0.0) + 1.0)
    big = w > 1.3
    ratio = jnp.where(big, 0.875, jnp.where(w > 0.5, 1.0, 0.0))
    phi_rows[...] = slope_scale * ratio / root
    rows[3] = root

    def gather(value):
        total = value[:, :WIDE]
        for start in range(WIDE, lanes, WIDE):
            total = total + value[:, start : start + WIDE]
        step = WIDE // 2
        while step >= slots:
            total = total + pltpu.roll(total, step, 1)
            step //= 2
        return total

    def fold(line):
        return gather(jnp.where(cell_mask, jnp.broadcast_to(line, (nz, lanes)), 0.0))

    for x, y in own_columns:
        t = (x - 1) * ny + y - 1
        pad_phi[x, y, base : base + nz, :] = fold(phi_rows[t : t + 1, :])

    copies_phi = start_exchange(pad_phi, send_phi, recv_phi)

    energy = rows[1] * (energy_scale * w) - 0.25 * w * w
    a_coef = jnp.where(big, 1.4, jnp.where(w > 0.5, 1.0, 0.0))
    rows[3] = energy - a_coef * rows[3]
    lax.fori_loop(0, nx * ny * 9, slopes, 0)

    arrive(copies_phi, 0, 0)
    expand_phi(own_columns)
    work(force, own_columns, True)
    for side in SIDES:
        arrive(copies_phi, *side)
        expand_phi(halo_columns(*side))
        work(force, halo_columns(*side), False)

    for x, y in own_columns:
        t = (x - 1) * ny + y - 1
        sums = [
            acc_force[t, (3 * k) * nz : (3 * k + 1) * nz]
            + acc_force[t, (3 * k + 1) * nz : (3 * k + 2) * nz]
            + acc_force[t, (3 * k + 2) * nz : (3 * k + 3) * nz]
            for k in range(4)
        ]
        scale = force_scale * own[t, 3]
        lines = [gather((sums[k] - own[t, k] * sums[3]) * scale) for k in range(3)]
        out_ref[x - 1, y - 1] = choose(lines + [fold(rows[3, t : t + 1, :])])

    for direction in DIRECTIONS:
        copies[direction].wait_send()
        copies_phi[direction].wait_send()


def body(axis_sizes, positions, types):
    nx, ny, nz, slots = types.shape
    lanes = nz * slots
    tall = 3 * slots
    count = len(DIRECTIONS)
    columns = nx * ny
    deep = 16 + nz
    f32, bf16 = jnp.float32, jnp.bfloat16
    return pl.pallas_call(
        functools.partial(kernel, (nx, ny, nz, slots), axis_sizes),
        out_shape=jax.ShapeDtypeStruct((nx, ny, nz, 4 * slots), f32),
        in_specs=[pl.BlockSpec(memory_space=pl.ANY), pl.BlockSpec(memory_space=pl.ANY)],
        out_specs=pl.BlockSpec(memory_space=pltpu.VMEM),
        scratch_shapes=[
            pltpu.VMEM((nx, ny, nz, 3 * slots), f32),
            pltpu.VMEM((nx, ny, nz, slots), jnp.int32),
            pltpu.VMEM((nx + 2, ny + 2, deep, WIDE), f32),
            pltpu.VMEM((nx + 2, ny + 2, deep, WIDE), f32),
            pltpu.VMEM((nx + 2, ny + 2, tall, DEEP), bf16),
            pltpu.VMEM((columns, DEEP, lanes), bf16),
            pltpu.VMEM((nx + 2, ny + 2, 12 * nz, 2 * WIDE), bf16),
            pltpu.VMEM((nx + 2, ny + 2, tall, lanes), f32),
            pltpu.VMEM((nx + 2, ny + 2, tall, lanes), f32),
            pltpu.VMEM((columns, 4, nz, lanes), f32),
            pltpu.VMEM((columns, 2, 8, lanes), f32),
            pltpu.VMEM((columns, 12 * nz, lanes), f32),
            pltpu.VMEM((4, columns, lanes), f32),
            pltpu.VMEM((columns, lanes), f32),
            pltpu.VMEM((DEEP, lanes), bf16),
            pltpu.VMEM((columns * 9, tall, lanes), f32),
            pltpu.VMEM((columns * 9, tall, lanes), f32),
            pltpu.SemaphoreType.DMA((2,)),
            pltpu.SemaphoreType.DMA((count,)),
            pltpu.SemaphoreType.DMA((count,)),
            pltpu.SemaphoreType.DMA((count,)),
            pltpu.SemaphoreType.DMA((count,)),
        ],
        compiler_params=pltpu.CompilerParams(
            collective_id=0, has_side_effects=True, vmem_limit_bytes=60 * 1024 * 1024
        ),
    )(positions, types)


def solution(mesh):
    spec = P("gx", "gy", "gz", None)
    sizes = tuple(mesh.shape[axis] for axis in AXES)
    return jax.shard_map(
        functools.partial(body, sizes),
        mesh=mesh,
        in_specs=(spec, spec),
        out_specs=spec,
        check_vma=False,
    )
```

```python
import functools
import math

import jax
import jax.numpy as jnp
from jax import lax
from jax.experimental import pallas as pl
from jax.experimental.pallas import tpu as pltpu
from jax.sharding import PartitionSpec as P

cut_square = 0.9025
density_rate = 3.0
unit = density_rate * math.log2(math.e)
alpha = math.sqrt(unit)
kappa = unit * cut_square
tail = 2.0**-kappa
shift_big = 2.0 * kappa / (cut_square * density_rate)
density_scale = tail / kappa**2
energy_scale = 0.25 * tail**2 / kappa**2
force_scale = -2.0 * tail**2 * density_rate / (kappa**2 * alpha)
slope_scale = -0.5 / tail
far = 1.0e4

AXES = ("gx", "gy", "gz")
DIRECTIONS = sorted(
    (
        (a, b, c)
        for a in (-1, 0, 1)
        for b in (-1, 0, 1)
        for c in (-1, 0, 1)
        if (a, b, c) != (0, 0, 0)
    ),
    key=lambda d: -(2 * abs(d[0]) + 2 * abs(d[1]) + abs(d[2])),
)
BATCHES = [
    [(-1, 0), (1, 0), (0, -1), (0, 1)],
    [(-1, -1), (-1, 1), (1, -1), (1, 1)],
]
WIDE = 128
DEEP = 256


def kernel(dims, axis_sizes, pos_ref, typ_ref, out_ref, pos, typ, pad, pad_phi, left, left_z, right, moment,
           spread_w, spread_z, spread_phi, own, acc, acc_force, rows, phi_rows, hot, pair_a, pair_b,
           load_sem, send_sem, recv_sem, send_phi, recv_phi):
    nx, ny, nz, slots = dims
    lanes = nz * slots
    tall = 3 * slots
    base = 8
    f32, bf16 = jnp.float32, jnp.bfloat16
    me = [lax.axis_index(axis) for axis in AXES]

    def peer(direction):
        return {
            axis: lax.rem(place + step + size, size)
            for axis, place, step, size in zip(AXES, me, direction, axis_sizes)
        }

    barrier = pltpu.get_barrier_semaphore()
    for direction in DIRECTIONS:
        pl.semaphore_signal(
            barrier, inc=1, device_id=peer(direction), device_id_type=pl.DeviceIdType.MESH
        )
    loads = [
        pltpu.make_async_copy(pos_ref, pos, load_sem.at[0]),
        pltpu.make_async_copy(typ_ref, typ, load_sem.at[1]),
    ]
    for load in loads:
        load.start()

    cell_mask = (
        lax.broadcasted_iota(jnp.int32, (nz, lanes), 1) // slots
        == lax.broadcasted_iota(jnp.int32, (nz, lanes), 0)
    )
    cells = jnp.where(cell_mask, 1.0, 0.0).astype(f32)
    group = lax.broadcasted_iota(jnp.int32, (nz, WIDE), 1) // slots
    empty = jnp.zeros((nz, lanes), f32)
    full = jnp.ones((nz, WIDE), f32)
    none = jnp.zeros((nz, WIDE), f32)
    parts = DEEP // nz
    used = 27
    hot[...] = jnp.concatenate(
        [empty] * (used - 3) + [cells] * 3 + [empty] * (parts - used), axis=0
    ).astype(bf16)

    for load in loads:
        load.wait()
    for x in range(nx):
        for y in range(ny):
            kind = typ[x, y]
            weight = jnp.where(kind == 1, 1.0, jnp.where(kind == 2, 1.6, 0.0)).astype(f32)
            pad[x + 1, y + 1, base : base + nz, :] = jnp.concatenate(
                [pos[x, y] * alpha, weight], axis=1
            )

    def pieces(value):
        high = value.astype(bf16).astype(f32)
        rest = value - high
        middle = rest.astype(bf16).astype(f32)
        return high, middle, rest - middle

    def choose(values):
        result = values[-1]
        for k in reversed(range(len(values) - 1)):
            result = jnp.where(group == k, values[k], result)
        return result

    def turn(value, step):
        step = (step * slots) % WIDE
        return pltpu.roll(value, step, 1) if step else value

    def centre(k, place):
        return (place - 0.5 * ((nx, ny)[k] + 1) - 0.5) * alpha

    layer = (jnp.minimum(group, 2).astype(f32) - 1.5) * alpha

    cell_row = lax.broadcasted_iota(jnp.int32, (nz, WIDE), 0)
    outside = ((group == 0) & (cell_row == 0)) | ((group == 2) & (cell_row == nz - 1))

    def neighbour(x, y, part):
        if part == "inner":
            middle = pad[x, y, base : base + nz, :]
            shifted = [
                jnp.where(cell_row == 0, 0.0, pltpu.roll(middle, 1, 0)),
                middle,
                jnp.where(cell_row == nz - 1, 0.0, pltpu.roll(middle, nz - 1, 0)),
            ]
        else:
            shifted = [pad[x, y, base - 1 + dz : base - 1 + dz + nz, :] for dz in range(3)]
        places = (0, 1, 2, 2)
        px, py, pz, w = (
            choose([turn(shifted[dz], g - q) for g, dz in enumerate(places)]) for q in range(4)
        )
        px = px + centre(0, x)
        py = py + centre(1, y)
        pz = pz + layer
        square = px * px + py * py + pz * pz
        present = w > 0.0
        if part == "outer":
            present = present & outside
        square = jnp.where(present, square, far)
        lines = []
        for value in (px, py, pz):
            h, m, l = pieces(value)
            lines += [h, m, h, l, m, h]
        lines += list(pieces(-square)) + [full] * 3
        ws = list(pieces(w))
        lines += ws + [none] * (parts - used)
        stacked = jnp.concatenate(lines, axis=0).astype(bf16).T
        if part == "outer":
            t = (x - 1) * ny + y - 1
            left_z[t, :slots] = stacked[:slots]
            left_z[t, slots:] = stacked[2 * slots : tall]
        else:
            left[x, y] = stacked[:tall]
        if part != "inner":
            terms = []
            for value in (w * px, w * py, w * pz):
                terms += list(pieces(value))
            moment[x, y] = jnp.concatenate(terms + ws, axis=0).astype(bf16)

    def spread_weight(x, y, part):
        if part == "outer":
            t = (x - 1) * ny + y - 1
            spread_z[t] = jnp.dot(left_z[t], hot[...], preferred_element_type=f32)
        else:
            spread_w[x, y] = jnp.dot(left[x, y], hot[...], preferred_element_type=f32)

    def owner(x, y):
        t = (x - 1) * ny + y - 1
        value = pad[x, y, base : base + nz, :]
        px, py, pz, w = (choose([turn(value, g - q) for g in range(WIDE // slots)]) for q in range(4))
        px = px + centre(0, x)
        py = py + centre(1, y)
        pz = pz - 0.5 * alpha
        square = kappa - (px * px + py * py + pz * pz)

        def tile(value):
            return jnp.where(cell_mask, jnp.concatenate([value] * (lanes // WIDE), axis=1), 0.0)

        lines = []
        for value in (px, py, pz):
            h, m, l = (tile(2.0 * piece) for piece in pieces(value))
            lines += [h, h, m, h, m, l]
        lines += [cells] * 3 + [tile(piece) for piece in pieces(square)]
        lines += [empty] * (parts - used + 3)
        right[t] = jnp.concatenate(lines, axis=0).astype(bf16)
        for k, value in enumerate((px, py, pz, w)):
            own[t, k] = tile(value)
        rows[2, t : t + 1, :] = jnp.sum(own[t, 3], axis=0, keepdims=True)

    def pair(x, y, a, b):
        return (((x - 1) * ny + y - 1) * 3 + a) * 3 + b

    def density(x, y, offsets, fresh):
        t = (x - 1) * ny + y - 1
        zero = jnp.zeros((8, lanes), f32)
        rho, energy = (zero, zero) if fresh else (acc[t, 0], acc[t, 1])
        for a, b in offsets:
            n = pair(x, y, a, b)
            column = (x + a - 1, y + b - 1)
            margin = jnp.dot(left[column], right[t], preferred_element_type=f32)
            for r in range(0, tall, 8):
                m = jnp.maximum(margin[r : r + 8], 0.0)
                u = jnp.exp2(m) * m
                q = u * spread_w[column[0], column[1], r : r + 8, :]
                rho = rho + q * m
                energy = energy + q * u
                pair_a[n, r : r + 8, :] = m
        acc[t, 0] = rho
        acc[t, 1] = energy

    def density_outer(x, y, offsets, fresh):
        t = (x - 1) * ny + y - 1
        ends = [(0, 0, slice(0, WIDE)), (slots, 2 * slots, slice(lanes - WIDE, lanes))]
        sums = [[acc[t, k, :, where] for k in range(2)] for _, _, where in ends]
        for a, b in offsets:
            n = pair(x, y, a, b)
            other = (x + a - 2) * ny + y + b - 2
            margin = jnp.dot(left_z[other], right[t], preferred_element_type=f32)
            for (start, place, where), total in zip(ends, sums):
                for r in range(0, slots, 8):
                    m = jnp.maximum(margin[start + r : start + r + 8, where], 0.0)
                    u = jnp.exp2(m) * m
                    q = u * spread_z[other, start + r : start + r + 8, where]
                    total[0] = total[0] + q * m
                    total[1] = total[1] + q * u
                    rows_at = slice(place + r, place + r + 8)
                    pair_a[n, rows_at, where] = pair_a[n, rows_at, where] + m
        for (_, _, where), total in zip(ends, sums):
            for k in range(2):
                acc[t, k, :, where] = total[k]

    def slopes(n, carry):
        for r in range(0, tall, 8):
            m = pair_a[n, r : r + 8, :]
            e = jnp.exp2(m)
            u = e * m
            pair_a[n, r : r + 8, :] = u * (m + shift_big)
            pair_b[n, r : r + 8, :] = u * (e * (m + 0.5 * shift_big))
        return carry

    def force(x, y, offsets, fresh):
        t = (x - 1) * ny + y - 1
        phi = jnp.broadcast_to(phi_rows[t : t + 1, :], (slots, lanes))
        total = None
        for a, b in offsets:
            n = pair(x, y, a, b)
            column = (x + a - 1, y + b - 1)
            high, low = [], []
            for r in range(0, tall, slots):
                both = phi + spread_phi[column[0], column[1], r : r + slots, :]
                v = both * pair_a[n, r : r + slots, :] + pair_b[n, r : r + slots, :]
                top = v.astype(bf16)
                high.append(top)
                low.append((v - top.astype(f32)).astype(bf16))
            values = jnp.concatenate(high + [low[2], low[0], low[1]], axis=0)
            terms = moment[column]
            terms = jnp.concatenate([terms, terms[:, : 2 * slots]], axis=1)
            part = jnp.dot(terms, values, preferred_element_type=f32)
            total = part if total is None else total + part
        acc_force[t] = total if fresh else acc_force[t] + total

    def halo_columns(a, b):
        xs = range(1, nx + 1) if a == 0 else [0 if a < 0 else nx + 1]
        ys = range(1, ny + 1) if b == 0 else [0 if b < 0 else ny + 1]
        return [(x, y) for x in xs for y in ys]

    own_columns = halo_columns(0, 0)

    def work(function, columns, fresh):
        for x, y in own_columns:
            offsets = [
                (a, b)
                for a in range(3)
                for b in range(3)
                if (x + a - 1, y + b - 1) in columns
            ]
            if offsets:
                function(x, y, offsets, fresh)

    many = WIDE // slots

    def expand_phi(columns):
        wide = [
            choose(
                [pad_phi[x, y, base - 1 + dz : base - 1 + dz + nz, :] for dz in range(3)]
            )
            for x, y in columns
        ]
        wide = wide[0] if len(wide) == 1 else jnp.concatenate(wide, axis=1)
        stacked = jnp.concatenate(pieces(wide), axis=0).astype(bf16)
        result = lax.dot_general(
            stacked,
            hot[(used - 3) * nz : used * nz, :],
            (((0,), (0,)), ((), ())),
            preferred_element_type=f32,
        )
        for k, (x, y) in enumerate(columns):
            spread_phi[x, y] = result[k * WIDE : k * WIDE + tall]

    def start_exchange(buffer, send, recv):
        def source(step, length):
            return (
                pl.ds(length, 1) if step > 0 else pl.ds(1, 1) if step < 0 else pl.ds(1, length)
            )

        def target(step, length):
            return (
                pl.ds(0, 1)
                if step > 0
                else pl.ds(length + 1, 1) if step < 0 else pl.ds(1, length)
            )

        def source_z(step):
            return (
                pl.ds(base + nz - 1, 1)
                if step > 0
                else pl.ds(base, 1) if step < 0 else pl.ds(base, nz)
            )

        def target_z(step):
            return (
                pl.ds(base - 1, 1)
                if step > 0
                else pl.ds(base + nz, 1) if step < 0 else pl.ds(base, nz)
            )

        copies = {}
        for index, direction in enumerate(DIRECTIONS):
            a, b, c = direction
            copy = pltpu.make_async_remote_copy(
                src_ref=buffer.at[source(a, nx), source(b, ny), source_z(c)],
                dst_ref=buffer.at[target(a, nx), target(b, ny), target_z(c)],
                send_sem=send.at[index],
                recv_sem=recv.at[index],
                device_id=peer(direction),
                device_id_type=pl.DeviceIdType.MESH,
            )
            copy.start()
            copies[direction] = copy
        return copies

    def arrive(copies, a, b):
        for c in (0, -1, 1):
            if (a, b, c) != (0, 0, 0):
                copies[(-a, -b, -c)].wait_recv()

    for x, y in own_columns:
        owner(x, y)
        neighbour(x, y, "inner")
    for x, y in own_columns:
        spread_weight(x, y, "inner")
    work(density, own_columns, True)

    pl.semaphore_wait(barrier, len(DIRECTIONS))
    copies = start_exchange(pad, send_sem, recv_sem)
    arrive(copies, 0, 0)
    for x, y in own_columns:
        neighbour(x, y, "outer")
    for x, y in own_columns:
        spread_weight(x, y, "outer")
    work(density_outer, own_columns, False)
    for sides in BATCHES:
        for side in sides:
            arrive(copies, *side)
        columns = [column for side in sides for column in halo_columns(*side)]
        for x, y in columns:
            neighbour(x, y, "all")
        for x, y in columns:
            spread_weight(x, y, "all")
        work(density, columns, False)

    for t in range(nx * ny):
        for k in range(2):
            rows[k, t : t + 1, :] = jnp.sum(acc[t, k], axis=0, keepdims=True)
    w = rows[2]
    rho = rows[0] * density_scale - w
    root = jnp.sqrt(jnp.maximum(rho, 0.0) + 1.0)
    big = w > 1.3
    ratio = jnp.where(big, 0.875, jnp.where(w > 0.5, 1.0, 0.0))
    phi_rows[...] = slope_scale * ratio / root
    rows[3] = root

    def gather(value):
        total = value[:, :WIDE]
        for start in range(WIDE, lanes, WIDE):
            total = total + value[:, start : start + WIDE]
        step = WIDE // 2
        while step >= slots:
            total = total + pltpu.roll(total, step, 1)
            step //= 2
        return total

    def fold(line):
        return gather(jnp.where(cell_mask, jnp.broadcast_to(line, (nz, lanes)), 0.0))

    for x, y in own_columns:
        t = (x - 1) * ny + y - 1
        pad_phi[x, y, base : base + nz, :] = fold(phi_rows[t : t + 1, :])

    copies_phi = start_exchange(pad_phi, send_phi, recv_phi)

    energy = rows[1] * (energy_scale * w) - 0.25 * w * w
    a_coef = jnp.where(big, 1.4, jnp.where(w > 0.5, 1.0, 0.0))
    rows[3] = energy - a_coef * rows[3]
    lax.fori_loop(0, nx * ny * 9, slopes, 0)

    arrive(copies_phi, 0, 0)
    expand_phi(own_columns)
    work(force, own_columns, True)
    for sides in BATCHES:
        for side in sides:
            arrive(copies_phi, *side)
        columns = [column for side in sides for column in halo_columns(*side)]
        expand_phi(columns)
        work(force, columns, False)

    for x, y in own_columns:
        t = (x - 1) * ny + y - 1
        sums = [
            acc_force[t, (3 * k) * nz : (3 * k + 1) * nz]
            + acc_force[t, (3 * k + 1) * nz : (3 * k + 2) * nz]
            + acc_force[t, (3 * k + 2) * nz : (3 * k + 3) * nz]
            for k in range(4)
        ]
        scale = force_scale * own[t, 3]
        lines = [gather((sums[k] - own[t, k] * sums[3]) * scale) for k in range(3)]
        out_ref[x - 1, y - 1] = choose(lines + [fold(rows[3, t : t + 1, :])])

    for direction in DIRECTIONS:
        copies[direction].wait_send()
        copies_phi[direction].wait_send()


def body(axis_sizes, positions, types):
    nx, ny, nz, slots = types.shape
    lanes = nz * slots
    tall = 3 * slots
    count = len(DIRECTIONS)
    columns = nx * ny
    deep = 16 + nz
    f32, bf16 = jnp.float32, jnp.bfloat16
    return pl.pallas_call(
        functools.partial(kernel, (nx, ny, nz, slots), axis_sizes),
        out_shape=pltpu.VMEM((nx, ny, nz, 4 * slots), f32),
        in_specs=[pl.BlockSpec(memory_space=pl.ANY), pl.BlockSpec(memory_space=pl.ANY)],
        out_specs=pl.BlockSpec(memory_space=pltpu.VMEM),
        scratch_shapes=[
            pltpu.VMEM((nx, ny, nz, 3 * slots), f32),
            pltpu.VMEM((nx, ny, nz, slots), jnp.int32),
            pltpu.VMEM((nx + 2, ny + 2, deep, WIDE), f32),
            pltpu.VMEM((nx + 2, ny + 2, deep, WIDE), f32),
            pltpu.VMEM((nx + 2, ny + 2, tall, DEEP), bf16),
            pltpu.VMEM((columns, 2 * slots, DEEP), bf16),
            pltpu.VMEM((columns, DEEP, lanes), bf16),
            pltpu.VMEM((nx + 2, ny + 2, 12 * nz, WIDE), bf16),
            pltpu.VMEM((nx + 2, ny + 2, tall, lanes), f32),
            pltpu.VMEM((columns, 2 * slots, lanes), f32),
            pltpu.VMEM((nx + 2, ny + 2, tall, lanes), f32),
            pltpu.VMEM((columns, 4, nz, lanes), f32),
            pltpu.VMEM((columns, 2, 8, lanes), f32),
            pltpu.VMEM((columns, 12 * nz, lanes), f32),
            pltpu.VMEM((4, columns, lanes), f32),
            pltpu.VMEM((columns, lanes), f32),
            pltpu.VMEM((DEEP, lanes), bf16),
            pltpu.VMEM((columns * 9, tall, lanes), f32),
            pltpu.VMEM((columns * 9, tall, lanes), f32),
            pltpu.SemaphoreType.DMA((2,)),
            pltpu.SemaphoreType.DMA((count,)),
            pltpu.SemaphoreType.DMA((count,)),
            pltpu.SemaphoreType.DMA((count,)),
            pltpu.SemaphoreType.DMA((count,)),
        ],
        compiler_params=pltpu.CompilerParams(
            collective_id=0, has_side_effects=True, vmem_limit_bytes=60 * 1024 * 1024
        ),
    )(positions, types)


def solution(mesh):
    spec = P("gx", "gy", "gz", None)
    sizes = tuple(mesh.shape[axis] for axis in AXES)
    return jax.shard_map(
        functools.partial(body, sizes),
        mesh=mesh,
        in_specs=(spec, spec),
        out_specs=spec,
        check_vma=False,
    )
```

```python
import functools
import math

import jax
import jax.numpy as jnp
from jax import lax
from jax.experimental import pallas as pl
from jax.experimental.pallas import tpu as pltpu
from jax.sharding import PartitionSpec as P

cut_square = 0.9025
density_rate = 3.0
unit = density_rate * math.log2(math.e)
alpha = math.sqrt(unit)
kappa = unit * cut_square
tail = 2.0**-kappa
shift_big = 2.0 * kappa / (cut_square * density_rate)
density_scale = tail / kappa**2
energy_scale = 0.25 * tail**2 / kappa**2
force_scale = -2.0 * tail**2 * density_rate / (kappa**2 * alpha)
slope_scale = -0.5 / tail
far = 1.0e4

AXES = ("gx", "gy", "gz")
DIRECTIONS = sorted(
    (
        (a, b, c)
        for a in (-1, 0, 1)
        for b in (-1, 0, 1)
        for c in (-1, 0, 1)
        if (a, b, c) != (0, 0, 0)
    ),
    key=lambda d: -(2 * abs(d[0]) + 2 * abs(d[1]) + abs(d[2])),
)
SIDES = [(-1, 0), (1, 0), (0, -1), (0, 1)]
CORNERS = [(-1, -1), (-1, 1), (1, -1), (1, 1)]


def stage(direction):
    return abs(direction[0]) + abs(direction[1])


WIDE = 128
DEEP = 256


def kernel(dims, axis_sizes, pos_ref, typ_ref, out_ref, pos, typ, pad, pad_phi, left, left_z, right, moment,
           spread_w, spread_z, spread_phi, own, acc, acc_force, rows, phi_rows, hot, pair_a, pair_b,
           blank, load_sem, send_sem, recv_sem, recv_phi):
    nx, ny, nz, slots = dims
    lanes = nz * slots
    tall = 3 * slots
    base = 8
    f32, bf16 = jnp.float32, jnp.bfloat16
    me = [lax.axis_index(axis) for axis in AXES]

    def peer(direction):
        return {
            axis: lax.rem(place + step + size, size)
            for axis, place, step, size in zip(AXES, me, direction, axis_sizes)
        }

    barrier = pltpu.get_barrier_semaphore()
    for direction in DIRECTIONS:
        pl.semaphore_signal(
            barrier, inc=1, device_id=peer(direction), device_id_type=pl.DeviceIdType.MESH
        )
    loads = [
        pltpu.make_async_copy(pos_ref, pos, load_sem.at[0]),
        pltpu.make_async_copy(typ_ref, typ, load_sem.at[1]),
    ]
    for load in loads:
        load.start()

    cell_mask = (
        lax.broadcasted_iota(jnp.int32, (nz, lanes), 1) // slots
        == lax.broadcasted_iota(jnp.int32, (nz, lanes), 0)
    )
    cells = jnp.where(cell_mask, 1.0, 0.0).astype(f32)
    group = lax.broadcasted_iota(jnp.int32, (nz, WIDE), 1) // slots
    empty = jnp.zeros((nz, lanes), f32)
    full = jnp.ones((nz, WIDE), f32)
    none = jnp.zeros((nz, WIDE), f32)
    parts = DEEP // nz
    used = 27
    hot[...] = jnp.concatenate(
        [empty] * (used - 3) + [cells] * 3 + [empty] * (parts - used), axis=0
    ).astype(bf16)

    for load in loads:
        load.wait()
    for x in range(nx):
        for y in range(ny):
            kind = typ[x, y]
            weight = jnp.where(kind == 1, 1.0, jnp.where(kind == 2, 1.6, 0.0)).astype(f32)
            pad[x + 1, y + 1, base : base + nz, :] = jnp.concatenate(
                [pos[x, y] * alpha, weight], axis=1
            )

    def pieces(value):
        high = value.astype(bf16).astype(f32)
        rest = value - high
        middle = rest.astype(bf16).astype(f32)
        return high, middle, rest - middle

    def choose(values):
        result = values[-1]
        for k in reversed(range(len(values) - 1)):
            result = jnp.where(group == k, values[k], result)
        return result

    def turn(value, step):
        step = (step * slots) % WIDE
        return pltpu.roll(value, step, 1) if step else value

    def centre(k, place):
        return (place - 0.5 * ((nx, ny)[k] + 1) - 0.5) * alpha

    layer = (jnp.minimum(group, 2).astype(f32) - 1.5) * alpha

    cell_row = lax.broadcasted_iota(jnp.int32, (nz, WIDE), 0)
    outside = ((group == 0) & (cell_row == 0)) | ((group == 2) & (cell_row == nz - 1))

    def neighbour(x, y, part):
        if part == "inner":
            middle = pad[x, y, base : base + nz, :]
            shifted = [
                jnp.where(cell_row == 0, 0.0, pltpu.roll(middle, 1, 0)),
                middle,
                jnp.where(cell_row == nz - 1, 0.0, pltpu.roll(middle, nz - 1, 0)),
            ]
        else:
            shifted = [pad[x, y, base - 1 + dz : base - 1 + dz + nz, :] for dz in range(3)]
        places = (0, 1, 2, 2)
        px, py, pz, w = (
            choose([turn(shifted[dz], g - q) for g, dz in enumerate(places)]) for q in range(4)
        )
        px = px + centre(0, x)
        py = py + centre(1, y)
        pz = pz + layer
        square = px * px + py * py + pz * pz
        present = w > 0.0
        if part == "outer":
            present = present & outside
        square = jnp.where(present, square, far)
        lines = []
        for value in (px, py, pz):
            h, m, l = pieces(value)
            lines += [h, m, h, l, m, h]
        lines += list(pieces(-square)) + [full] * 3
        ws = list(pieces(w))
        lines += ws + [none] * (parts - used)
        stacked = jnp.concatenate(lines, axis=0).astype(bf16).T
        if part == "outer":
            t = (x - 1) * ny + y - 1
            left_z[t, :slots] = stacked[:slots]
            left_z[t, slots:] = stacked[2 * slots : tall]
        else:
            left[x, y] = stacked[:tall]
        if part != "inner":
            terms = []
            for value in (w * px, w * py, w * pz):
                terms += list(pieces(value))
            moment[x, y] = jnp.concatenate(terms + ws, axis=0).astype(bf16)

    def spread_weight(x, y, part):
        if part == "outer":
            t = (x - 1) * ny + y - 1
            spread_z[t] = jnp.dot(left_z[t], hot[...], preferred_element_type=f32)
        else:
            spread_w[x, y] = jnp.dot(left[x, y], hot[...], preferred_element_type=f32)

    def owner(x, y):
        t = (x - 1) * ny + y - 1
        value = pad[x, y, base : base + nz, :]
        px, py, pz, w = (choose([turn(value, g - q) for g in range(WIDE // slots)]) for q in range(4))
        px = px + centre(0, x)
        py = py + centre(1, y)
        pz = pz - 0.5 * alpha
        square = kappa - (px * px + py * py + pz * pz)

        def tile(value):
            return jnp.where(cell_mask, jnp.concatenate([value] * (lanes // WIDE), axis=1), 0.0)

        lines = []
        for value in (px, py, pz):
            h, m, l = (tile(2.0 * piece) for piece in pieces(value))
            lines += [h, h, m, h, m, l]
        lines += [cells] * 3 + [tile(piece) for piece in pieces(square)]
        lines += [empty] * (parts - used + 3)
        right[t] = jnp.concatenate(lines, axis=0).astype(bf16)
        for k, value in enumerate((px, py, pz, w)):
            own[t, k] = tile(value)
        rows[2, t : t + 1, :] = jnp.sum(own[t, 3], axis=0, keepdims=True)

    def pair(x, y, a, b):
        return (((x - 1) * ny + y - 1) * 3 + a) * 3 + b

    def density(x, y, offsets, fresh):
        t = (x - 1) * ny + y - 1
        zero = jnp.zeros((8, lanes), f32)
        rho, energy = (zero, zero) if fresh else (acc[t, 0], acc[t, 1])
        for a, b in offsets:
            n = pair(x, y, a, b)
            column = (x + a - 1, y + b - 1)
            margin = jnp.dot(left[column], right[t], preferred_element_type=f32)
            for r in range(0, tall, 8):
                m = jnp.maximum(margin[r : r + 8], 0.0)
                u = jnp.exp2(m) * m
                q = u * spread_w[column[0], column[1], r : r + 8, :]
                rho = rho + q * m
                energy = energy + q * u
                pair_a[n, r : r + 8, :] = m
        acc[t, 0] = rho
        acc[t, 1] = energy

    def density_outer(x, y, offsets, fresh):
        t = (x - 1) * ny + y - 1
        ends = [(0, 0, slice(0, WIDE)), (slots, 2 * slots, slice(lanes - WIDE, lanes))]
        sums = [[acc[t, k, :, where] for k in range(2)] for _, _, where in ends]
        for a, b in offsets:
            n = pair(x, y, a, b)
            other = (x + a - 2) * ny + y + b - 2
            margin = jnp.dot(left_z[other], right[t], preferred_element_type=f32)
            for (start, place, where), total in zip(ends, sums):
                for r in range(0, slots, 8):
                    m = jnp.maximum(margin[start + r : start + r + 8, where], 0.0)
                    u = jnp.exp2(m) * m
                    q = u * spread_z[other, start + r : start + r + 8, where]
                    total[0] = total[0] + q * m
                    total[1] = total[1] + q * u
                    rows_at = slice(place + r, place + r + 8)
                    pair_a[n, rows_at, where] = pair_a[n, rows_at, where] + m
        for (_, _, where), total in zip(ends, sums):
            for k in range(2):
                acc[t, k, :, where] = total[k]

    def slopes(n):
        for r in range(0, tall, 8):
            m = pair_a[n, r : r + 8, :]
            e = jnp.exp2(m)
            u = e * m
            pair_a[n, r : r + 8, :] = u * (m + shift_big)
            pair_b[n, r : r + 8, :] = u * (e * (m + 0.5 * shift_big))

    def force(x, y, offsets, fresh):
        t = (x - 1) * ny + y - 1
        phi = jnp.broadcast_to(phi_rows[t : t + 1, :], (slots, lanes))
        total = None
        for a, b in offsets:
            n = pair(x, y, a, b)
            column = (x + a - 1, y + b - 1)
            high, low = [], []
            for r in range(0, tall, slots):
                both = phi + spread_phi[column[0], column[1], r : r + slots, :]
                if fresh:
                    m = pair_a[n, r : r + slots, :]
                    e = jnp.exp2(m)
                    v = (e * m) * (both * (m + shift_big) + e * (m + 0.5 * shift_big))
                else:
                    v = both * pair_a[n, r : r + slots, :] + pair_b[n, r : r + slots, :]
                top = v.astype(bf16)
                high.append(top)
                low.append((v - top.astype(f32)).astype(bf16))
            values = jnp.concatenate(high + [low[2], low[0], low[1]], axis=0)
            terms = moment[column]
            terms = jnp.concatenate([terms, terms[:, : 2 * slots]], axis=1)
            part = jnp.dot(terms, values, preferred_element_type=f32)
            total = part if total is None else total + part
        acc_force[t] = total if fresh else acc_force[t] + total

    def halo_columns(a, b):
        xs = range(1, nx + 1) if a == 0 else [0 if a < 0 else nx + 1]
        ys = range(1, ny + 1) if b == 0 else [0 if b < 0 else ny + 1]
        return [(x, y) for x in xs for y in ys]

    own_columns = halo_columns(0, 0)
    side_columns = [column for side in SIDES for column in halo_columns(*side)]
    corner_columns = [column for side in CORNERS for column in halo_columns(*side)]

    def work(function, columns, fresh):
        for x, y in own_columns:
            offsets = [
                (a, b)
                for a in range(3)
                for b in range(3)
                if (x + a - 1, y + b - 1) in columns
            ]
            if offsets:
                function(x, y, offsets, fresh)

    many = WIDE // slots

    def expand_phi(columns):
        wide = [
            choose(
                [pad_phi[x, y, base - 1 + dz : base - 1 + dz + nz, :] for dz in range(3)]
            )
            for x, y in columns
        ]
        wide = wide[0] if len(wide) == 1 else jnp.concatenate(wide, axis=1)
        stacked = jnp.concatenate(pieces(wide), axis=0).astype(bf16)
        result = lax.dot_general(
            stacked,
            hot[(used - 3) * nz : used * nz, :],
            (((0,), (0,)), ((), ())),
            preferred_element_type=f32,
        )
        for k, (x, y) in enumerate(columns):
            spread_phi[x, y] = result[k * WIDE : k * WIDE + tall]

    def start_exchange(buffer, send, recv):
        def source(step, length):
            return (
                pl.ds(length, 1) if step > 0 else pl.ds(1, 1) if step < 0 else pl.ds(1, length)
            )

        def target(step, length):
            return (
                pl.ds(0, 1)
                if step > 0
                else pl.ds(length + 1, 1) if step < 0 else pl.ds(1, length)
            )

        def source_z(step):
            return (
                pl.ds(base + nz - 1, 1)
                if step > 0
                else pl.ds(base, 1) if step < 0 else pl.ds(base, nz)
            )

        def target_z(step):
            return (
                pl.ds(base - 1, 1)
                if step > 0
                else pl.ds(base + nz, 1) if step < 0 else pl.ds(base, nz)
            )

        for direction in DIRECTIONS:
            a, b, c = direction
            pltpu.make_async_remote_copy(
                src_ref=buffer.at[source(a, nx), source(b, ny), source_z(c)],
                dst_ref=buffer.at[target(a, nx), target(b, ny), target_z(c)],
                send_sem=send,
                recv_sem=recv.at[stage(direction)],
                device_id=peer(direction),
                device_id_type=pl.DeviceIdType.MESH,
            ).start()

    def await_rows(directions, semaphore):
        count = sum(
            (1 if a else nx) * (1 if b else ny) * (1 if c else nz) for a, b, c in directions
        )
        part = blank.at[pl.ds(0, count)]
        pltpu.make_async_copy(part, part, semaphore).wait()

    def arrive(recv, number):
        await_rows([d for d in DIRECTIONS if stage(d) == number], recv.at[number])

    for x, y in own_columns:
        owner(x, y)
        neighbour(x, y, "inner")
    for x, y in own_columns:
        spread_weight(x, y, "inner")

    pl.semaphore_wait(barrier, len(DIRECTIONS))
    start_exchange(pad, send_sem.at[0], recv_sem)
    work(density, own_columns, True)
    arrive(recv_sem, 0)
    for x, y in own_columns:
        neighbour(x, y, "outer")
    for x, y in own_columns:
        spread_weight(x, y, "outer")
    work(density_outer, own_columns, False)
    arrive(recv_sem, 1)
    arrive(recv_sem, 2)
    columns = side_columns + corner_columns
    for x, y in columns:
        neighbour(x, y, "all")
    for x, y in columns:
        spread_weight(x, y, "all")
    work(density, columns, False)

    for t in range(nx * ny):
        for k in range(2):
            rows[k, t : t + 1, :] = jnp.sum(acc[t, k], axis=0, keepdims=True)
    w = rows[2]
    rho = rows[0] * density_scale - w
    root = jnp.sqrt(jnp.maximum(rho, 0.0) + 1.0)
    big = w > 1.3
    ratio = jnp.where(big, 0.875, jnp.where(w > 0.5, 1.0, 0.0))
    phi_rows[...] = slope_scale * ratio / root
    rows[3] = root

    def gather(value):
        total = value[:, :WIDE]
        for start in range(WIDE, lanes, WIDE):
            total = total + value[:, start : start + WIDE]
        step = WIDE // 2
        while step >= slots:
            total = total + pltpu.roll(total, step, 1)
            step //= 2
        return total

    def fold(line):
        return gather(jnp.where(cell_mask, jnp.broadcast_to(line, (nz, lanes)), 0.0))

    for x, y in own_columns:
        t = (x - 1) * ny + y - 1
        pad_phi[x, y, base : base + nz, :] = fold(phi_rows[t : t + 1, :])

    start_exchange(pad_phi, send_sem.at[1], recv_phi)

    energy = rows[1] * (energy_scale * w) - 0.25 * w * w
    a_coef = jnp.where(big, 1.4, jnp.where(w > 0.5, 1.0, 0.0))
    rows[3] = energy - a_coef * rows[3]
    for x, y in own_columns:
        for a in range(3):
            for b in range(3):
                if (x + a - 1, y + b - 1) not in own_columns:
                    slopes(pair(x, y, a, b))

    arrive(recv_phi, 0)
    expand_phi(own_columns)
    work(force, own_columns, True)
    arrive(recv_phi, 1)
    expand_phi(side_columns)
    work(force, side_columns, False)
    arrive(recv_phi, 2)
    expand_phi(corner_columns)
    work(force, corner_columns, False)

    for x, y in own_columns:
        t = (x - 1) * ny + y - 1
        sums = [
            acc_force[t, (3 * k) * nz : (3 * k + 1) * nz]
            + acc_force[t, (3 * k + 1) * nz : (3 * k + 2) * nz]
            + acc_force[t, (3 * k + 2) * nz : (3 * k + 3) * nz]
            for k in range(4)
        ]
        scale = force_scale * own[t, 3]
        lines = [gather((sums[k] - own[t, k] * sums[3]) * scale) for k in range(3)]
        out_ref[x - 1, y - 1] = choose(lines + [fold(rows[3, t : t + 1, :])])

    for number in range(2):
        await_rows(DIRECTIONS, send_sem.at[number])


def body(axis_sizes, positions, types):
    nx, ny, nz, slots = types.shape
    lanes = nz * slots
    tall = 3 * slots
    columns = nx * ny
    deep = 16 + nz
    f32, bf16 = jnp.float32, jnp.bfloat16
    return pl.pallas_call(
        functools.partial(kernel, (nx, ny, nz, slots), axis_sizes),
        out_shape=pltpu.VMEM((nx, ny, nz, 4 * slots), f32),
        in_specs=[pl.BlockSpec(memory_space=pl.ANY), pl.BlockSpec(memory_space=pl.ANY)],
        out_specs=pl.BlockSpec(memory_space=pltpu.VMEM),
        scratch_shapes=[
            pltpu.VMEM((nx, ny, nz, 3 * slots), f32),
            pltpu.VMEM((nx, ny, nz, slots), jnp.int32),
            pltpu.VMEM((nx + 2, ny + 2, deep, WIDE), f32),
            pltpu.VMEM((nx + 2, ny + 2, deep, WIDE), f32),
            pltpu.VMEM((nx + 2, ny + 2, tall, DEEP), bf16),
            pltpu.VMEM((columns, 2 * slots, DEEP), bf16),
            pltpu.VMEM((columns, DEEP, lanes), bf16),
            pltpu.VMEM((nx + 2, ny + 2, 12 * nz, WIDE), bf16),
            pltpu.VMEM((nx + 2, ny + 2, tall, lanes), f32),
            pltpu.VMEM((columns, 2 * slots, lanes), f32),
            pltpu.VMEM((nx + 2, ny + 2, tall, lanes), f32),
            pltpu.VMEM((columns, 4, nz, lanes), f32),
            pltpu.VMEM((columns, 2, 8, lanes), f32),
            pltpu.VMEM((columns, 12 * nz, lanes), f32),
            pltpu.VMEM((4, columns, lanes), f32),
            pltpu.VMEM((columns, lanes), f32),
            pltpu.VMEM((DEEP, lanes), bf16),
            pltpu.VMEM((columns * 9, tall, lanes), f32),
            pltpu.VMEM((columns * 9, tall, lanes), f32),
            pltpu.VMEM(((nx + 2) * (ny + 2) * nz, WIDE), f32),
            pltpu.SemaphoreType.DMA((2,)),
            pltpu.SemaphoreType.DMA((2,)),
            pltpu.SemaphoreType.DMA((3,)),
            pltpu.SemaphoreType.DMA((3,)),
        ],
        compiler_params=pltpu.CompilerParams(
            collective_id=0, has_side_effects=True, vmem_limit_bytes=60 * 1024 * 1024
        ),
    )(positions, types)


def solution(mesh):
    spec = P("gx", "gy", "gz", None)
    sizes = tuple(mesh.shape[axis] for axis in AXES)
    return jax.shard_map(
        functools.partial(body, sizes),
        mesh=mesh,
        in_specs=(spec, spec),
        out_specs=spec,
        check_vma=False,
    )
```

```python
import functools
import math

import jax
import jax.numpy as jnp
from jax import lax
from jax.experimental import pallas as pl
from jax.experimental.pallas import tpu as pltpu
from jax.sharding import PartitionSpec as P

cut_square = 0.9025
density_rate = 3.0
unit = density_rate * math.log2(math.e)
alpha = math.sqrt(unit)
kappa = unit * cut_square
tail = 2.0**-kappa
shift_big = 2.0 * kappa / (cut_square * density_rate)
density_scale = tail / kappa**2
energy_scale = 0.25 * tail**2 / kappa**2
force_scale = -2.0 * tail**2 * density_rate / (kappa**2 * alpha)
slope_scale = -0.5 / tail
far = 1.0e4

AXES = ("gx", "gy", "gz")
DIRECTIONS = sorted(
    (
        (a, b, c)
        for a in (-1, 0, 1)
        for b in (-1, 0, 1)
        for c in (-1, 0, 1)
        if (a, b, c) != (0, 0, 0)
    ),
    key=lambda d: -(2 * abs(d[0]) + 2 * abs(d[1]) + abs(d[2])),
)
SIDES = [(-1, 0), (1, 0), (0, -1), (0, 1)]
CORNERS = [(-1, -1), (-1, 1), (1, -1), (1, 1)]


def stage(direction):
    return abs(direction[0]) + abs(direction[1])


WIDE = 128
DEEP = 256


def kernel(dims, axis_sizes, pos_ref, typ_ref, out_ref, pos, typ, pad, pad_phi, left, left_z, right, moment,
           spread_w, spread_z, spread_phi, own, acc, acc_force, rows, phi_rows, hot, pair_a, pair_b,
           blank, load_sem, send_sem, recv_sem, recv_phi):
    nx, ny, nz, slots = dims
    lanes = nz * slots
    tall = 3 * slots
    base = 8
    f32, bf16 = jnp.float32, jnp.bfloat16
    me = [lax.axis_index(axis) for axis in AXES]

    def peer(direction):
        return {
            axis: lax.rem(place + step + size, size)
            for axis, place, step, size in zip(AXES, me, direction, axis_sizes)
        }

    barrier = pltpu.get_barrier_semaphore()
    for direction in DIRECTIONS:
        pl.semaphore_signal(
            barrier, inc=1, device_id=peer(direction), device_id_type=pl.DeviceIdType.MESH
        )
    loads = [
        pltpu.make_async_copy(pos_ref, pos, load_sem.at[0]),
        pltpu.make_async_copy(typ_ref, typ, load_sem.at[1]),
    ]
    for load in loads:
        load.start()

    cell_mask = (
        lax.broadcasted_iota(jnp.int32, (nz, lanes), 1) // slots
        == lax.broadcasted_iota(jnp.int32, (nz, lanes), 0)
    )
    cells = jnp.where(cell_mask, 1.0, 0.0).astype(f32)
    group = lax.broadcasted_iota(jnp.int32, (nz, WIDE), 1) // slots
    empty = jnp.zeros((nz, lanes), f32)
    full = jnp.ones((nz, WIDE), f32)
    none = jnp.zeros((nz, WIDE), f32)
    parts = DEEP // nz
    used = 27
    hot[...] = jnp.concatenate(
        [empty] * (used - 3) + [cells] * 3 + [empty] * (parts - used), axis=0
    ).astype(bf16)

    for load in loads:
        load.wait()
    for x in range(nx):
        for y in range(ny):
            kind = typ[x, y]
            weight = jnp.where(kind == 1, 1.0, jnp.where(kind == 2, 1.6, 0.0)).astype(f32)
            pad[x + 1, y + 1, base : base + nz, :] = jnp.concatenate(
                [pos[x, y] * alpha, weight], axis=1
            )

    def pieces(value):
        high = value.astype(bf16).astype(f32)
        rest = value - high
        middle = rest.astype(bf16).astype(f32)
        return high, middle, rest - middle

    def choose(values):
        result = values[-1]
        for k in reversed(range(len(values) - 1)):
            result = jnp.where(group == k, values[k], result)
        return result

    def turn(value, step):
        step = (step * slots) % WIDE
        return pltpu.roll(value, step, 1) if step else value

    def centre(k, place):
        return (place - 0.5 * ((nx, ny)[k] + 1) - 0.5) * alpha

    layer = (jnp.minimum(group, 2).astype(f32) - 1.5) * alpha

    cell_row = lax.broadcasted_iota(jnp.int32, (nz, WIDE), 0)
    outside = ((group == 0) & (cell_row == 0)) | ((group == 2) & (cell_row == nz - 1))

    def neighbour(x, y, part):
        if part == "inner":
            middle = pad[x, y, base : base + nz, :]
            shifted = [
                jnp.where(cell_row == 0, 0.0, pltpu.roll(middle, 1, 0)),
                middle,
                jnp.where(cell_row == nz - 1, 0.0, pltpu.roll(middle, nz - 1, 0)),
            ]
        else:
            shifted = [pad[x, y, base - 1 + dz : base - 1 + dz + nz, :] for dz in range(3)]
        places = (0, 1, 2, 2)
        px, py, pz, w = (
            choose([turn(shifted[dz], g - q) for g, dz in enumerate(places)]) for q in range(4)
        )
        px = px + centre(0, x)
        py = py + centre(1, y)
        pz = pz + layer
        square = px * px + py * py + pz * pz
        present = w > 0.0
        if part == "outer":
            present = present & outside
        square = jnp.where(present, square, far)
        lines = []
        for value in (px, py, pz):
            h, m, l = pieces(value)
            lines += [h, m, h, l, m, h]
        lines += list(pieces(-square)) + [full] * 3
        ws = list(pieces(w))
        lines += ws + [none] * (parts - used)
        stacked = jnp.concatenate(lines, axis=0).astype(bf16).T
        if part == "outer":
            t = (x - 1) * ny + y - 1
            left_z[t, :slots] = stacked[:slots]
            left_z[t, slots:] = stacked[2 * slots : tall]
        else:
            left[x, y] = stacked[:tall]
        if part != "inner":
            terms = []
            for value in (w * px, w * py, w * pz):
                terms += list(pieces(value))
            moment[x, y] = jnp.concatenate(terms + ws, axis=0).astype(bf16)

    def spread_weight(x, y, part):
        if part == "outer":
            t = (x - 1) * ny + y - 1
            spread_z[t] = jnp.dot(left_z[t], hot[...], preferred_element_type=f32)
        else:
            spread_w[x, y] = jnp.dot(left[x, y], hot[...], preferred_element_type=f32)

    def owner(x, y):
        t = (x - 1) * ny + y - 1
        value = pad[x, y, base : base + nz, :]
        px, py, pz, w = (choose([turn(value, g - q) for g in range(WIDE // slots)]) for q in range(4))
        px = px + centre(0, x)
        py = py + centre(1, y)
        pz = pz - 0.5 * alpha
        square = kappa - (px * px + py * py + pz * pz)

        def tile(value):
            return jnp.where(cell_mask, jnp.concatenate([value] * (lanes // WIDE), axis=1), 0.0)

        lines = []
        for value in (px, py, pz):
            h, m, l = (tile(2.0 * piece) for piece in pieces(value))
            lines += [h, h, m, h, m, l]
        lines += [cells] * 3 + [tile(piece) for piece in pieces(square)]
        lines += [empty] * (parts - used + 3)
        right[t] = jnp.concatenate(lines, axis=0).astype(bf16)
        for k, value in enumerate((px, py, pz, w)):
            own[t, k] = tile(value)
        rows[2, t : t + 1, :] = jnp.sum(own[t, 3], axis=0, keepdims=True)

    def pair(x, y, a, b):
        return (((x - 1) * ny + y - 1) * 3 + a) * 3 + b

    def density(x, y, offsets, fresh):
        t = (x - 1) * ny + y - 1
        zero = jnp.zeros((8, lanes), f32)
        rho, energy = (zero, zero) if fresh else (acc[t, 0], acc[t, 1])
        for a, b in offsets:
            n = pair(x, y, a, b)
            column = (x + a - 1, y + b - 1)
            margin = jnp.dot(left[column], right[t], preferred_element_type=f32)
            for r in range(0, tall, 8):
                m = jnp.maximum(margin[r : r + 8], 0.0)
                u = jnp.exp2(m) * m
                q = u * spread_w[column[0], column[1], r : r + 8, :]
                rho = rho + q * m
                energy = energy + q * u
                pair_a[n, r : r + 8, :] = m
        acc[t, 0] = rho
        acc[t, 1] = energy

    def density_outer(x, y, offsets, fresh):
        t = (x - 1) * ny + y - 1
        ends = [(0, 0, slice(0, WIDE)), (slots, 2 * slots, slice(lanes - WIDE, lanes))]
        sums = [[acc[t, k, :, where] for k in range(2)] for _, _, where in ends]
        for a, b in offsets:
            n = pair(x, y, a, b)
            other = (x + a - 2) * ny + y + b - 2
            margin = jnp.dot(left_z[other], right[t], preferred_element_type=f32)
            for (start, place, where), total in zip(ends, sums):
                for r in range(0, slots, 8):
                    m = jnp.maximum(margin[start + r : start + r + 8, where], 0.0)
                    u = jnp.exp2(m) * m
                    q = u * spread_z[other, start + r : start + r + 8, where]
                    total[0] = total[0] + q * m
                    total[1] = total[1] + q * u
                    rows_at = slice(place + r, place + r + 8)
                    pair_a[n, rows_at, where] = pair_a[n, rows_at, where] + m
        for (_, _, where), total in zip(ends, sums):
            for k in range(2):
                acc[t, k, :, where] = total[k]

    def slopes(n):
        for r in range(0, tall, 8):
            m = pair_a[n, r : r + 8, :]
            e = jnp.exp2(m)
            u = e * m
            pair_a[n, r : r + 8, :] = u * (m + shift_big)
            pair_b[n, r : r + 8, :] = u * (e * (m + 0.5 * shift_big))

    def force(x, y, offsets, fresh):
        t = (x - 1) * ny + y - 1
        phi = jnp.broadcast_to(phi_rows[t : t + 1, :], (slots, lanes))
        total = None
        for a, b in offsets:
            n = pair(x, y, a, b)
            column = (x + a - 1, y + b - 1)
            high, low = [], []
            for r in range(0, tall, slots):
                both = phi + spread_phi[column[0], column[1], r : r + slots, :]
                if fresh:
                    m = pair_a[n, r : r + slots, :]
                    e = jnp.exp2(m)
                    v = (e * m) * (both * (m + shift_big) + e * (m + 0.5 * shift_big))
                else:
                    v = both * pair_a[n, r : r + slots, :] + pair_b[n, r : r + slots, :]
                top = v.astype(bf16)
                high.append(top)
                low.append((v - top.astype(f32)).astype(bf16))
            values = jnp.concatenate(high + [low[2], low[0], low[1]], axis=0)
            terms = moment[column]
            terms = jnp.concatenate([terms, terms[:, : 2 * slots]], axis=1)
            part = jnp.dot(terms, values, preferred_element_type=f32)
            total = part if total is None else total + part
        acc_force[t] = total if fresh else acc_force[t] + total

    def halo_columns(a, b):
        xs = range(1, nx + 1) if a == 0 else [0 if a < 0 else nx + 1]
        ys = range(1, ny + 1) if b == 0 else [0 if b < 0 else ny + 1]
        return [(x, y) for x in xs for y in ys]

    own_columns = halo_columns(0, 0)
    side_columns = [column for side in SIDES for column in halo_columns(*side)]
    corner_columns = [column for side in CORNERS for column in halo_columns(*side)]

    def work(function, columns, fresh):
        for x, y in own_columns:
            offsets = [
                (a, b)
                for a in range(3)
                for b in range(3)
                if (x + a - 1, y + b - 1) in columns
            ]
            if offsets:
                function(x, y, offsets, fresh)

    many = WIDE // slots

    def expand_phi(columns):
        wide = [
            choose(
                [pad_phi[x, y, base - 1 + dz : base - 1 + dz + nz, :] for dz in range(3)]
            )
            for x, y in columns
        ]
        wide = wide[0] if len(wide) == 1 else jnp.concatenate(wide, axis=1)
        stacked = jnp.concatenate(pieces(wide), axis=0).astype(bf16)
        result = lax.dot_general(
            stacked,
            hot[(used - 3) * nz : used * nz, :],
            (((0,), (0,)), ((), ())),
            preferred_element_type=f32,
        )
        for k, (x, y) in enumerate(columns):
            spread_phi[x, y] = result[k * WIDE : k * WIDE + tall]

    def start_exchange(buffer, send, recv):
        def source(step, length):
            return (
                pl.ds(length, 1) if step > 0 else pl.ds(1, 1) if step < 0 else pl.ds(1, length)
            )

        def target(step, length):
            return (
                pl.ds(0, 1)
                if step > 0
                else pl.ds(length + 1, 1) if step < 0 else pl.ds(1, length)
            )

        def source_z(step):
            return (
                pl.ds(base + nz - 1, 1)
                if step > 0
                else pl.ds(base, 1) if step < 0 else pl.ds(base, nz)
            )

        def target_z(step):
            return (
                pl.ds(base - 1, 1)
                if step > 0
                else pl.ds(base + nz, 1) if step < 0 else pl.ds(base, nz)
            )

        for direction in DIRECTIONS:
            a, b, c = direction
            pltpu.make_async_remote_copy(
                src_ref=buffer.at[source(a, nx), source(b, ny), source_z(c)],
                dst_ref=buffer.at[target(a, nx), target(b, ny), target_z(c)],
                send_sem=send,
                recv_sem=recv.at[stage(direction)],
                device_id=peer(direction),
                device_id_type=pl.DeviceIdType.MESH,
            ).start()

    def await_rows(directions, semaphore):
        count = sum(
            (1 if a else nx) * (1 if b else ny) * (1 if c else nz) for a, b, c in directions
        )
        part = blank.at[pl.ds(0, count)]
        pltpu.make_async_copy(part, part, semaphore).wait()

    def arrive(recv, number):
        await_rows([d for d in DIRECTIONS if stage(d) == number], recv.at[number])

    always = me[0] >= 0
    early = (me[0] + 1) // 2 + me[1] < 3

    def region(condition):
        return lambda function: pl.when(condition)(function)

    for x, y in own_columns:
        owner(x, y)

    def own_inner():
        for x, y in own_columns:
            neighbour(x, y, "inner")
        for x, y in own_columns:
            spread_weight(x, y, "inner")
        work(density, own_columns, True)

    region(early)(own_inner)
    pl.semaphore_wait(barrier, len(DIRECTIONS))
    start_exchange(pad, send_sem.at[0], recv_sem)
    region(jnp.logical_not(early))(own_inner)

    @region(always)
    def own_outer():
        arrive(recv_sem, 0)
        for x, y in own_columns:
            neighbour(x, y, "outer")
        for x, y in own_columns:
            spread_weight(x, y, "outer")
        work(density_outer, own_columns, False)

    @region(always)
    def halo():
        arrive(recv_sem, 1)
        arrive(recv_sem, 2)
        columns = side_columns + corner_columns
        for x, y in columns:
            neighbour(x, y, "all")
        for x, y in columns:
            spread_weight(x, y, "all")
        work(density, columns, False)

    for t in range(nx * ny):
        for k in range(2):
            rows[k, t : t + 1, :] = jnp.sum(acc[t, k], axis=0, keepdims=True)
    w = rows[2]
    rho = rows[0] * density_scale - w
    root = jnp.sqrt(jnp.maximum(rho, 0.0) + 1.0)
    big = w > 1.3
    ratio = jnp.where(big, 0.875, jnp.where(w > 0.5, 1.0, 0.0))
    phi_rows[...] = slope_scale * ratio / root
    rows[3] = root

    def gather(value):
        total = value[:, :WIDE]
        for start in range(WIDE, lanes, WIDE):
            total = total + value[:, start : start + WIDE]
        step = WIDE // 2
        while step >= slots:
            total = total + pltpu.roll(total, step, 1)
            step //= 2
        return total

    def fold(line):
        return gather(jnp.where(cell_mask, jnp.broadcast_to(line, (nz, lanes)), 0.0))

    for x, y in own_columns:
        t = (x - 1) * ny + y - 1
        pad_phi[x, y, base : base + nz, :] = fold(phi_rows[t : t + 1, :])

    start_exchange(pad_phi, send_sem.at[1], recv_phi)

    @region(always)
    def between():
        w = rows[2]
        energy = rows[1] * (energy_scale * w) - 0.25 * w * w
        a_coef = jnp.where(w > 1.3, 1.4, jnp.where(w > 0.5, 1.0, 0.0))
        rows[3] = energy - a_coef * rows[3]
        for x, y in own_columns:
            for a in range(3):
                for b in range(3):
                    if (x + a - 1, y + b - 1) not in own_columns:
                        slopes(pair(x, y, a, b))

    @region(always)
    def own_force():
        arrive(recv_phi, 0)
        expand_phi(own_columns)
        work(force, own_columns, True)

    @region(always)
    def side_force():
        arrive(recv_phi, 1)
        expand_phi(side_columns)
        work(force, side_columns, False)

    arrive(recv_phi, 2)
    expand_phi(corner_columns)
    work(force, corner_columns, False)

    for x, y in own_columns:
        t = (x - 1) * ny + y - 1
        sums = [
            acc_force[t, (3 * k) * nz : (3 * k + 1) * nz]
            + acc_force[t, (3 * k + 1) * nz : (3 * k + 2) * nz]
            + acc_force[t, (3 * k + 2) * nz : (3 * k + 3) * nz]
            for k in range(4)
        ]
        scale = force_scale * own[t, 3]
        lines = [gather((sums[k] - own[t, k] * sums[3]) * scale) for k in range(3)]
        out_ref[x - 1, y - 1] = choose(lines + [fold(rows[3, t : t + 1, :])])

    for number in range(2):
        await_rows(DIRECTIONS, send_sem.at[number])


def body(axis_sizes, positions, types):
    nx, ny, nz, slots = types.shape
    lanes = nz * slots
    tall = 3 * slots
    columns = nx * ny
    deep = 16 + nz
    f32, bf16 = jnp.float32, jnp.bfloat16
    return pl.pallas_call(
        functools.partial(kernel, (nx, ny, nz, slots), axis_sizes),
        out_shape=pltpu.VMEM((nx, ny, nz, 4 * slots), f32),
        in_specs=[pl.BlockSpec(memory_space=pl.ANY), pl.BlockSpec(memory_space=pl.ANY)],
        out_specs=pl.BlockSpec(memory_space=pltpu.VMEM),
        scratch_shapes=[
            pltpu.VMEM((nx, ny, nz, 3 * slots), f32),
            pltpu.VMEM((nx, ny, nz, slots), jnp.int32),
            pltpu.VMEM((nx + 2, ny + 2, deep, WIDE), f32),
            pltpu.VMEM((nx + 2, ny + 2, deep, WIDE), f32),
            pltpu.VMEM((nx + 2, ny + 2, tall, DEEP), bf16),
            pltpu.VMEM((columns, 2 * slots, DEEP), bf16),
            pltpu.VMEM((columns, DEEP, lanes), bf16),
            pltpu.VMEM((nx + 2, ny + 2, 12 * nz, WIDE), bf16),
            pltpu.VMEM((nx + 2, ny + 2, tall, lanes), f32),
            pltpu.VMEM((columns, 2 * slots, lanes), f32),
            pltpu.VMEM((nx + 2, ny + 2, tall, lanes), f32),
            pltpu.VMEM((columns, 4, nz, lanes), f32),
            pltpu.VMEM((columns, 2, 8, lanes), f32),
            pltpu.VMEM((columns, 12 * nz, lanes), f32),
            pltpu.VMEM((4, columns, lanes), f32),
            pltpu.VMEM((columns, lanes), f32),
            pltpu.VMEM((DEEP, lanes), bf16),
            pltpu.VMEM((columns * 9, tall, lanes), f32),
            pltpu.VMEM((columns * 9, tall, lanes), f32),
            pltpu.VMEM(((nx + 2) * (ny + 2) * nz, WIDE), f32),
            pltpu.SemaphoreType.DMA((2,)),
            pltpu.SemaphoreType.DMA((2,)),
            pltpu.SemaphoreType.DMA((3,)),
            pltpu.SemaphoreType.DMA((3,)),
        ],
        compiler_params=pltpu.CompilerParams(
            collective_id=0, has_side_effects=True, vmem_limit_bytes=60 * 1024 * 1024
        ),
    )(positions, types)


def solution(mesh):
    spec = P("gx", "gy", "gz", None)
    sizes = tuple(mesh.shape[axis] for axis in AXES)
    return jax.shard_map(
        functools.partial(body, sizes),
        mesh=mesh,
        in_specs=(spec, spec),
        out_specs=spec,
        check_vma=False,
    )
```

```python
import functools
import math

import jax
import jax.numpy as jnp
from jax import lax
from jax.experimental import pallas as pl
from jax.experimental.pallas import tpu as pltpu
from jax.sharding import PartitionSpec as P

cut_square = 0.9025
density_rate = 3.0
unit = density_rate * math.log2(math.e)
alpha = math.sqrt(unit)
kappa = unit * cut_square
tail = 2.0**-kappa
shift_big = 2.0 * kappa / (cut_square * density_rate)
density_scale = tail / kappa**2
energy_scale = 0.25 * tail**2 / kappa**2
force_scale = -2.0 * tail**2 * density_rate / (kappa**2 * alpha)
slope_scale = -0.5 / tail
far = 1.0e4

AXES = ("gx", "gy", "gz")
DIRECTIONS = sorted(
    (
        (a, b, c)
        for a in (-1, 0, 1)
        for b in (-1, 0, 1)
        for c in (-1, 0, 1)
        if (a, b, c) != (0, 0, 0)
    ),
    key=lambda d: -(2 * abs(d[0]) + 2 * abs(d[1]) + abs(d[2])),
)
X_SIDES = [(-1, 0), (1, 0)]
Y_SIDES = [(0, -1), (0, 1)]
CORNERS = [(-1, -1), (-1, 1), (1, -1), (1, 1)]


def stage(direction):
    return abs(direction[0]) + 2 * abs(direction[1])


WIDE = 128
DEEP = 256


def kernel(dims, axis_sizes, pos_ref, typ_ref, out_ref, pos, typ, pad, pad_phi, left, left_z, right, moment,
           spread_w, spread_z, spread_phi, own, acc, acc_force, rows, phi_rows, hot, pair_a, pair_b,
           blank, load_sem, send_sem, recv_sem, recv_phi):
    nx, ny, nz, slots = dims
    lanes = nz * slots
    tall = 3 * slots
    base = 8
    f32, bf16 = jnp.float32, jnp.bfloat16
    me = [lax.axis_index(axis) for axis in AXES]

    def peer(direction):
        return {
            axis: lax.rem(place + step + size, size)
            for axis, place, step, size in zip(AXES, me, direction, axis_sizes)
        }

    barrier = pltpu.get_barrier_semaphore()
    for direction in DIRECTIONS:
        pl.semaphore_signal(
            barrier, inc=1, device_id=peer(direction), device_id_type=pl.DeviceIdType.MESH
        )
    loads = [
        pltpu.make_async_copy(pos_ref, pos, load_sem.at[0]),
        pltpu.make_async_copy(typ_ref, typ, load_sem.at[1]),
    ]
    for load in loads:
        load.start()

    cell_mask = (
        lax.broadcasted_iota(jnp.int32, (nz, lanes), 1) // slots
        == lax.broadcasted_iota(jnp.int32, (nz, lanes), 0)
    )
    cells = jnp.where(cell_mask, 1.0, 0.0).astype(f32)
    group = lax.broadcasted_iota(jnp.int32, (nz, WIDE), 1) // slots
    empty = jnp.zeros((nz, lanes), f32)
    full = jnp.ones((nz, WIDE), f32)
    none = jnp.zeros((nz, WIDE), f32)
    parts = DEEP // nz
    used = 27
    hot[...] = jnp.concatenate(
        [empty] * (used - 3) + [cells] * 3 + [empty] * (parts - used), axis=0
    ).astype(bf16)

    for load in loads:
        load.wait()
    for x in range(nx):
        for y in range(ny):
            kind = typ[x, y]
            weight = jnp.where(kind == 1, 1.0, jnp.where(kind == 2, 1.6, 0.0)).astype(f32)
            pad[x + 1, y + 1, base : base + nz, :] = jnp.concatenate(
                [pos[x, y] * alpha, weight], axis=1
            )

    def pieces(value):
        high = value.astype(bf16).astype(f32)
        rest = value - high
        middle = rest.astype(bf16).astype(f32)
        return high, middle, rest - middle

    def choose(values):
        result = values[-1]
        for k in reversed(range(len(values) - 1)):
            result = jnp.where(group == k, values[k], result)
        return result

    def turn(value, step):
        step = (step * slots) % WIDE
        return pltpu.roll(value, step, 1) if step else value

    def centre(k, place):
        return (place - 0.5 * ((nx, ny)[k] + 1) - 0.5) * alpha

    layer = (jnp.minimum(group, 2).astype(f32) - 1.5) * alpha

    cell_row = lax.broadcasted_iota(jnp.int32, (nz, WIDE), 0)
    outside = ((group == 0) & (cell_row == 0)) | ((group == 2) & (cell_row == nz - 1))

    def neighbour(x, y, part):
        if part == "inner":
            middle = pad[x, y, base : base + nz, :]
            shifted = [
                jnp.where(cell_row == 0, 0.0, pltpu.roll(middle, 1, 0)),
                middle,
                jnp.where(cell_row == nz - 1, 0.0, pltpu.roll(middle, nz - 1, 0)),
            ]
        else:
            shifted = [pad[x, y, base - 1 + dz : base - 1 + dz + nz, :] for dz in range(3)]
        places = (0, 1, 2, 2)
        px, py, pz, w = (
            choose([turn(shifted[dz], g - q) for g, dz in enumerate(places)]) for q in range(4)
        )
        px = px + centre(0, x)
        py = py + centre(1, y)
        pz = pz + layer
        square = px * px + py * py + pz * pz
        present = w > 0.0
        if part == "outer":
            present = present & outside
        square = jnp.where(present, square, far)
        lines = []
        for value in (px, py, pz):
            h, m, l = pieces(value)
            lines += [h, m, h, l, m, h]
        lines += list(pieces(-square)) + [full] * 3
        ws = list(pieces(w))
        lines += ws + [none] * (parts - used)
        stacked = jnp.concatenate(lines, axis=0).astype(bf16).T
        if part == "outer":
            t = (x - 1) * ny + y - 1
            left_z[t, :slots] = stacked[:slots]
            left_z[t, slots:] = stacked[2 * slots : tall]
        else:
            left[x, y] = stacked[:tall]
        if part != "inner":
            terms = []
            for value in (w * px, w * py, w * pz):
                terms += list(pieces(value))
            moment[x, y] = jnp.concatenate(terms + ws, axis=0).astype(bf16)

    def spread_weight(x, y, part):
        if part == "outer":
            t = (x - 1) * ny + y - 1
            spread_z[t] = jnp.dot(left_z[t], hot[...], preferred_element_type=f32)
        else:
            spread_w[x, y] = jnp.dot(left[x, y], hot[...], preferred_element_type=f32)

    def owner(x, y):
        t = (x - 1) * ny + y - 1
        value = pad[x, y, base : base + nz, :]
        px, py, pz, w = (choose([turn(value, g - q) for g in range(WIDE // slots)]) for q in range(4))
        px = px + centre(0, x)
        py = py + centre(1, y)
        pz = pz - 0.5 * alpha
        square = kappa - (px * px + py * py + pz * pz)

        def tile(value):
            return jnp.where(cell_mask, jnp.concatenate([value] * (lanes // WIDE), axis=1), 0.0)

        lines = []
        for value in (px, py, pz):
            h, m, l = (tile(2.0 * piece) for piece in pieces(value))
            lines += [h, h, m, h, m, l]
        lines += [cells] * 3 + [tile(piece) for piece in pieces(square)]
        lines += [empty] * (parts - used + 3)
        right[t] = jnp.concatenate(lines, axis=0).astype(bf16)
        for k, value in enumerate((px, py, pz, w)):
            own[t, k] = tile(value)
        rows[2, t : t + 1, :] = jnp.sum(own[t, 3], axis=0, keepdims=True)

    def pair(x, y, a, b):
        return (((x - 1) * ny + y - 1) * 3 + a) * 3 + b

    def density(x, y, offsets, fresh):
        t = (x - 1) * ny + y - 1
        zero = jnp.zeros((8, lanes), f32)
        rho, energy = (zero, zero) if fresh else (acc[t, 0], acc[t, 1])
        for a, b in offsets:
            n = pair(x, y, a, b)
            column = (x + a - 1, y + b - 1)
            margin = jnp.dot(left[column], right[t], preferred_element_type=f32)
            for r in range(0, tall, 8):
                m = jnp.maximum(margin[r : r + 8], 0.0)
                u = jnp.exp2(m) * m
                q = u * spread_w[column[0], column[1], r : r + 8, :]
                rho = rho + q * m
                energy = energy + q * u
                pair_a[n, r : r + 8, :] = m
        acc[t, 0] = rho
        acc[t, 1] = energy

    def density_outer(x, y, offsets, fresh):
        t = (x - 1) * ny + y - 1
        ends = [(0, 0, slice(0, WIDE)), (slots, 2 * slots, slice(lanes - WIDE, lanes))]
        sums = [[acc[t, k, :, where] for k in range(2)] for _, _, where in ends]
        for a, b in offsets:
            n = pair(x, y, a, b)
            other = (x + a - 2) * ny + y + b - 2
            margin = jnp.dot(left_z[other], right[t], preferred_element_type=f32)
            for (start, place, where), total in zip(ends, sums):
                for r in range(0, slots, 8):
                    m = jnp.maximum(margin[start + r : start + r + 8, where], 0.0)
                    u = jnp.exp2(m) * m
                    q = u * spread_z[other, start + r : start + r + 8, where]
                    total[0] = total[0] + q * m
                    total[1] = total[1] + q * u
                    rows_at = slice(place + r, place + r + 8)
                    pair_a[n, rows_at, where] = pair_a[n, rows_at, where] + m
        for (_, _, where), total in zip(ends, sums):
            for k in range(2):
                acc[t, k, :, where] = total[k]

    def slopes(n):
        for r in range(0, tall, 8):
            m = pair_a[n, r : r + 8, :]
            e = jnp.exp2(m)
            u = e * m
            pair_a[n, r : r + 8, :] = u * (m + shift_big)
            pair_b[n, r : r + 8, :] = u * (e * (m + 0.5 * shift_big))

    def force(x, y, offsets, fresh):
        t = (x - 1) * ny + y - 1
        phi = jnp.broadcast_to(phi_rows[t : t + 1, :], (slots, lanes))
        total = None
        for a, b in offsets:
            n = pair(x, y, a, b)
            column = (x + a - 1, y + b - 1)
            high, low = [], []
            for r in range(0, tall, slots):
                both = phi + spread_phi[column[0], column[1], r : r + slots, :]
                if fresh:
                    m = pair_a[n, r : r + slots, :]
                    e = jnp.exp2(m)
                    v = (e * m) * (both * (m + shift_big) + e * (m + 0.5 * shift_big))
                else:
                    v = both * pair_a[n, r : r + slots, :] + pair_b[n, r : r + slots, :]
                top = v.astype(bf16)
                high.append(top)
                low.append((v - top.astype(f32)).astype(bf16))
            values = jnp.concatenate(high + [low[2], low[0], low[1]], axis=0)
            terms = moment[column]
            terms = jnp.concatenate([terms, terms[:, : 2 * slots]], axis=1)
            part = jnp.dot(terms, values, preferred_element_type=f32)
            total = part if total is None else total + part
        acc_force[t] = total if fresh else acc_force[t] + total

    def halo_columns(a, b):
        xs = range(1, nx + 1) if a == 0 else [0 if a < 0 else nx + 1]
        ys = range(1, ny + 1) if b == 0 else [0 if b < 0 else ny + 1]
        return [(x, y) for x in xs for y in ys]

    own_columns = halo_columns(0, 0)
    x_columns, y_columns, corner_columns = (
        [column for side in sides for column in halo_columns(*side)]
        for sides in (X_SIDES, Y_SIDES, CORNERS)
    )
    last = [(x, y) for x in sorted({1, nx}) for y in sorted({1, ny})]
    first = [column for column in own_columns if column not in last]

    def work(function, columns, fresh):
        for x, y in own_columns:
            offsets = [
                (a, b)
                for a in range(3)
                for b in range(3)
                if (x + a - 1, y + b - 1) in columns
            ]
            if offsets:
                function(x, y, offsets, fresh)

    many = WIDE // slots

    def expand_phi(columns):
        wide = [
            choose(
                [pad_phi[x, y, base - 1 + dz : base - 1 + dz + nz, :] for dz in range(3)]
            )
            for x, y in columns
        ]
        wide = wide[0] if len(wide) == 1 else jnp.concatenate(wide, axis=1)
        stacked = jnp.concatenate(pieces(wide), axis=0).astype(bf16)
        result = lax.dot_general(
            stacked,
            hot[(used - 3) * nz : used * nz, :],
            (((0,), (0,)), ((), ())),
            preferred_element_type=f32,
        )
        for k, (x, y) in enumerate(columns):
            spread_phi[x, y] = result[k * WIDE : k * WIDE + tall]

    def start_exchange(buffer, send, recv):
        def source(step, length):
            return (
                pl.ds(length, 1) if step > 0 else pl.ds(1, 1) if step < 0 else pl.ds(1, length)
            )

        def target(step, length):
            return (
                pl.ds(0, 1)
                if step > 0
                else pl.ds(length + 1, 1) if step < 0 else pl.ds(1, length)
            )

        def source_z(step):
            return (
                pl.ds(base + nz - 1, 1)
                if step > 0
                else pl.ds(base, 1) if step < 0 else pl.ds(base, nz)
            )

        def target_z(step):
            return (
                pl.ds(base - 1, 1)
                if step > 0
                else pl.ds(base + nz, 1) if step < 0 else pl.ds(base, nz)
            )

        for direction in DIRECTIONS:
            a, b, c = direction
            pltpu.make_async_remote_copy(
                src_ref=buffer.at[source(a, nx), source(b, ny), source_z(c)],
                dst_ref=buffer.at[target(a, nx), target(b, ny), target_z(c)],
                send_sem=send,
                recv_sem=recv.at[stage(direction)],
                device_id=peer(direction),
                device_id_type=pl.DeviceIdType.MESH,
            ).start()

    def await_rows(directions, semaphore):
        count = sum(
            (1 if a else nx) * (1 if b else ny) * (1 if c else nz) for a, b, c in directions
        )
        part = blank.at[pl.ds(0, count)]
        pltpu.make_async_copy(part, part, semaphore).wait()

    def arrive(recv, number):
        await_rows([d for d in DIRECTIONS if stage(d) == number], recv.at[number])

    always = me[0] >= 0
    early = (me[0] + 1) // 2 + me[1] < 3

    def region(condition):
        return lambda function: pl.when(condition)(function)

    for x, y in own_columns:
        owner(x, y)

    def own_inner():
        for x, y in own_columns:
            neighbour(x, y, "inner")
        for x, y in own_columns:
            spread_weight(x, y, "inner")
        work(density, own_columns, True)

    region(early)(own_inner)
    pl.semaphore_wait(barrier, len(DIRECTIONS))
    start_exchange(pad, send_sem.at[0], recv_sem)
    region(jnp.logical_not(early))(own_inner)

    @region(always)
    def own_outer():
        arrive(recv_sem, 0)
        for x, y in own_columns:
            neighbour(x, y, "outer")
        for x, y in own_columns:
            spread_weight(x, y, "outer")
        work(density_outer, own_columns, False)

    def gather(value):
        total = value[:, :WIDE]
        for start in range(WIDE, lanes, WIDE):
            total = total + value[:, start : start + WIDE]
        step = WIDE // 2
        while step >= slots:
            total = total + pltpu.roll(total, step, 1)
            step //= 2
        return total

    def fold(line):
        return gather(jnp.where(cell_mask, jnp.broadcast_to(line, (nz, lanes)), 0.0))

    def halo(number, columns):
        arrive(recv_sem, number)
        for x, y in columns:
            neighbour(x, y, "all")
        for x, y in columns:
            spread_weight(x, y, "all")
        work(density, columns, False)

    def derivatives(columns):
        places = [(x - 1) * ny + y - 1 for x, y in columns]
        for t in places:
            for k in range(2):
                rows[k, t : t + 1, :] = jnp.sum(acc[t, k], axis=0, keepdims=True)
        rho, w = (
            jnp.concatenate([rows[k, t : t + 1, :] for t in places], axis=0) for k in (0, 2)
        )
        root = jnp.sqrt(jnp.maximum(rho * density_scale - w, 0.0) + 1.0)
        ratio = jnp.where(w > 1.3, 0.875, jnp.where(w > 0.5, 1.0, 0.0))
        phi = slope_scale * ratio / root
        for k, (t, (x, y)) in enumerate(zip(places, columns)):
            line = phi[k : k + 1]
            pad_phi[x, y, base : base + nz, :] = fold(line)
            phi_rows[t : t + 1, :] = line
            rows[3, t : t + 1, :] = root[k : k + 1]

    @region(always)
    def halo_x():
        halo(1, x_columns)

    @region(always)
    def halo_y():
        halo(2, y_columns)
        derivatives(first)

    @region(always)
    def halo_corners():
        halo(3, corner_columns)
        derivatives(last)

    start_exchange(pad_phi, send_sem.at[1], recv_phi)

    @region(always)
    def between():
        w = rows[2]
        energy = rows[1] * (energy_scale * w) - 0.25 * w * w
        a_coef = jnp.where(w > 1.3, 1.4, jnp.where(w > 0.5, 1.0, 0.0))
        rows[3] = energy - a_coef * rows[3]
        for x, y in own_columns:
            for a in range(3):
                for b in range(3):
                    if (x + a - 1, y + b - 1) not in own_columns:
                        slopes(pair(x, y, a, b))

    @region(always)
    def own_force():
        arrive(recv_phi, 0)
        expand_phi(own_columns)
        work(force, own_columns, True)

    def halo_force(number, columns):
        arrive(recv_phi, number)
        expand_phi(columns)
        work(force, columns, False)

    def write(columns):
        for x, y in columns:
            t = (x - 1) * ny + y - 1
            sums = [
                acc_force[t, (3 * k) * nz : (3 * k + 1) * nz]
                + acc_force[t, (3 * k + 1) * nz : (3 * k + 2) * nz]
                + acc_force[t, (3 * k + 2) * nz : (3 * k + 3) * nz]
                for k in range(4)
            ]
            scale = force_scale * own[t, 3]
            lines = [gather((sums[k] - own[t, k] * sums[3]) * scale) for k in range(3)]
            out_ref[x - 1, y - 1] = choose(lines + [fold(rows[3, t : t + 1, :])])

    @region(always)
    def force_x():
        halo_force(1, x_columns)

    @region(always)
    def force_y():
        halo_force(2, y_columns)
        write(first)

    halo_force(3, corner_columns)
    write(last)

    for number in range(2):
        await_rows(DIRECTIONS, send_sem.at[number])


def body(axis_sizes, positions, types):
    nx, ny, nz, slots = types.shape
    lanes = nz * slots
    tall = 3 * slots
    columns = nx * ny
    deep = 16 + nz
    f32, bf16 = jnp.float32, jnp.bfloat16
    return pl.pallas_call(
        functools.partial(kernel, (nx, ny, nz, slots), axis_sizes),
        out_shape=pltpu.VMEM((nx, ny, nz, 4 * slots), f32),
        in_specs=[pl.BlockSpec(memory_space=pl.ANY), pl.BlockSpec(memory_space=pl.ANY)],
        out_specs=pl.BlockSpec(memory_space=pltpu.VMEM),
        scratch_shapes=[
            pltpu.VMEM((nx, ny, nz, 3 * slots), f32),
            pltpu.VMEM((nx, ny, nz, slots), jnp.int32),
            pltpu.VMEM((nx + 2, ny + 2, deep, WIDE), f32),
            pltpu.VMEM((nx + 2, ny + 2, deep, WIDE), f32),
            pltpu.VMEM((nx + 2, ny + 2, tall, DEEP), bf16),
            pltpu.VMEM((columns, 2 * slots, DEEP), bf16),
            pltpu.VMEM((columns, DEEP, lanes), bf16),
            pltpu.VMEM((nx + 2, ny + 2, 12 * nz, WIDE), bf16),
            pltpu.VMEM((nx + 2, ny + 2, tall, lanes), f32),
            pltpu.VMEM((columns, 2 * slots, lanes), f32),
            pltpu.VMEM((nx + 2, ny + 2, tall, lanes), f32),
            pltpu.VMEM((columns, 4, nz, lanes), f32),
            pltpu.VMEM((columns, 2, 8, lanes), f32),
            pltpu.VMEM((columns, 12 * nz, lanes), f32),
            pltpu.VMEM((4, columns, lanes), f32),
            pltpu.VMEM((columns, lanes), f32),
            pltpu.VMEM((DEEP, lanes), bf16),
            pltpu.VMEM((columns * 9, tall, lanes), f32),
            pltpu.VMEM((columns * 9, tall, lanes), f32),
            pltpu.VMEM(((nx + 2) * (ny + 2) * nz, WIDE), f32),
            pltpu.SemaphoreType.DMA((2,)),
            pltpu.SemaphoreType.DMA((2,)),
            pltpu.SemaphoreType.DMA((4,)),
            pltpu.SemaphoreType.DMA((4,)),
        ],
        compiler_params=pltpu.CompilerParams(
            collective_id=0, has_side_effects=True, vmem_limit_bytes=60 * 1024 * 1024
        ),
    )(positions, types)


def solution(mesh):
    spec = P("gx", "gy", "gz", None)
    sizes = tuple(mesh.shape[axis] for axis in AXES)
    return jax.shard_map(
        functools.partial(body, sizes),
        mesh=mesh,
        in_specs=(spec, spec),
        out_specs=spec,
        check_vma=False,
    )
```

```python
import functools
import math

import jax
import jax.numpy as jnp
from jax import lax
from jax.experimental import pallas as pl
from jax.experimental.pallas import tpu as pltpu
from jax.sharding import PartitionSpec as P

cut_square = 0.9025
density_rate = 3.0
unit = density_rate * math.log2(math.e)
alpha = math.sqrt(unit)
kappa = unit * cut_square
tail = 2.0**-kappa
shift_big = 2.0 * kappa / (cut_square * density_rate)
density_scale = tail / kappa**2
energy_scale = 0.25 * tail**2 / kappa**2
force_scale = -2.0 * tail**2 * density_rate / (kappa**2 * alpha)
slope_scale = -0.5 / tail
far = 1.0e4

AXES = ("gx", "gy", "gz")
DIRECTIONS = sorted(
    (
        (a, b, c)
        for a in (-1, 0, 1)
        for b in (-1, 0, 1)
        for c in (-1, 0, 1)
        if (a, b, c) != (0, 0, 0)
    ),
    key=lambda d: -(2 * abs(d[0]) + 2 * abs(d[1]) + abs(d[2])),
)
def stage(direction):
    a, b, _ = direction
    return 2 + (b > 0) if b else abs(a)


WIDE = 128
DEEP = 256


def kernel(dims, axis_sizes, pos_ref, typ_ref, out_ref, pos, typ, pad, pad_phi, left, left_z, right, moment,
           moment_phi, weighted, spread_w, spread_z, spread_phi, own, acc, acc_force, rows, phi_rows, hot, pair_a, pair_s,
           blank, load_sem, send_sem, recv_sem, recv_phi):
    nx, ny, nz, slots = dims
    lanes = nz * slots
    tall = 3 * slots
    base = 8
    f32, bf16 = jnp.float32, jnp.bfloat16
    me = [lax.axis_index(axis) for axis in AXES]

    def peer(direction):
        return {
            axis: lax.rem(place + step + size, size)
            for axis, place, step, size in zip(AXES, me, direction, axis_sizes)
        }

    barrier = pltpu.get_barrier_semaphore()
    for direction in DIRECTIONS:
        pl.semaphore_signal(
            barrier, inc=1, device_id=peer(direction), device_id_type=pl.DeviceIdType.MESH
        )
    loads = [
        pltpu.make_async_copy(pos_ref, pos, load_sem.at[0]),
        pltpu.make_async_copy(typ_ref, typ, load_sem.at[1]),
    ]
    for load in loads:
        load.start()

    cell_mask = (
        lax.broadcasted_iota(jnp.int32, (nz, lanes), 1) // slots
        == lax.broadcasted_iota(jnp.int32, (nz, lanes), 0)
    )
    cells = jnp.where(cell_mask, 1.0, 0.0).astype(f32)
    group = lax.broadcasted_iota(jnp.int32, (nz, WIDE), 1) // slots
    empty = jnp.zeros((nz, lanes), f32)
    full = jnp.ones((nz, WIDE), f32)
    none = jnp.zeros((nz, WIDE), f32)
    parts = DEEP // nz
    used = 27
    hot[...] = jnp.concatenate(
        [empty] * (used - 3) + [cells] * 3 + [empty] * (parts - used), axis=0
    ).astype(bf16)

    for load in loads:
        load.wait()
    for x in range(nx):
        for y in range(ny):
            kind = typ[x, y]
            weight = jnp.where(kind == 1, 1.0, jnp.where(kind == 2, 1.6, 0.0)).astype(f32)
            pad[x + 1, y + 1, base : base + nz, :] = jnp.concatenate(
                [pos[x, y] * alpha, weight], axis=1
            )

    def pieces(value):
        high = value.astype(bf16).astype(f32)
        rest = value - high
        middle = rest.astype(bf16).astype(f32)
        return high, middle, rest - middle

    def choose(values):
        result = values[-1]
        for k in reversed(range(len(values) - 1)):
            result = jnp.where(group == k, values[k], result)
        return result

    def turn(value, step):
        step = (step * slots) % WIDE
        return pltpu.roll(value, step, 1) if step else value

    def centre(k, place):
        return (jnp.asarray(place, f32) - (0.5 * ((nx, ny)[k] + 1) + 0.5)) * alpha

    layer = (jnp.minimum(group, 2).astype(f32) - 1.5) * alpha

    cell_row = lax.broadcasted_iota(jnp.int32, (nz, WIDE), 0)
    outside = ((group == 0) & (cell_row == 0)) | ((group == 2) & (cell_row == nz - 1))

    def neighbour(x, y, part):
        if part == "inner":
            middle = pad[x, y, base : base + nz, :]
            shifted = [
                jnp.where(cell_row == 0, 0.0, pltpu.roll(middle, 1, 0)),
                middle,
                jnp.where(cell_row == nz - 1, 0.0, pltpu.roll(middle, nz - 1, 0)),
            ]
        else:
            shifted = [pad[x, y, base - 1 + dz : base - 1 + dz + nz, :] for dz in range(3)]
        places = (0, 1, 2, 2)
        px, py, pz, w = (
            choose([turn(shifted[dz], g - q) for g, dz in enumerate(places)]) for q in range(4)
        )
        px = px + centre(0, x)
        py = py + centre(1, y)
        pz = pz + layer
        square = px * px + py * py + pz * pz
        present = w > 0.0
        if part == "outer":
            present = present & outside
        square = jnp.where(present, square, far)
        lines = []
        for value in (px, py, pz):
            h, m, l = pieces(value)
            lines += [h, m, h, l, m, h]
        lines += list(pieces(-square)) + [full] * 3
        ws = list(pieces(w))
        lines += ws + [none] * (parts - used)
        stacked = jnp.concatenate(lines, axis=0).astype(bf16).T
        if part == "outer":
            t = (x - 1) * ny + y - 1
            left_z[t, :slots] = stacked[:slots]
            left_z[t, slots:] = stacked[2 * slots : tall]
        else:
            left[x, y] = stacked[:tall]
        if part != "inner":
            values = (w * px, w * py, w * pz)
            terms = []
            for k, value in enumerate(values):
                terms += list(pieces(value))
                weighted[x, y, k] = value
            weighted[x, y, 3] = w
            moment[x, y] = jnp.concatenate(terms + ws, axis=0).astype(bf16)

    def spread_weight(x, y, part):
        if part == "outer":
            t = (x - 1) * ny + y - 1
            spread_z[t] = jnp.dot(left_z[t], hot[...], preferred_element_type=f32)
        else:
            spread_w[x, y] = jnp.dot(left[x, y], hot[...], preferred_element_type=f32)

    def owner(x, y):
        t = (x - 1) * ny + y - 1
        value = pad[x, y, base : base + nz, :]
        px, py, pz, w = (choose([turn(value, g - q) for g in range(WIDE // slots)]) for q in range(4))
        px = px + centre(0, x)
        py = py + centre(1, y)
        pz = pz - 0.5 * alpha
        square = kappa - (px * px + py * py + pz * pz)

        def tile(value):
            return jnp.where(cell_mask, jnp.concatenate([value] * (lanes // WIDE), axis=1), 0.0)

        lines = []
        for value in (px, py, pz):
            h, m, l = (tile(2.0 * piece) for piece in pieces(value))
            lines += [h, h, m, h, m, l]
        lines += [cells] * 3 + [tile(piece) for piece in pieces(square)]
        lines += [empty] * (parts - used + 3)
        right[t] = jnp.concatenate(lines, axis=0).astype(bf16)
        for k, value in enumerate((px, py, pz, w)):
            own[t, k] = tile(value)
        rows[2, t] = jnp.sum(own[t, 3], axis=0, keepdims=True)

    def pair(x, y, a, b):
        return (((x - 1) * ny + y - 1) * 3 + a) * 3 + b

    def margins(operands, t):
        step = 3
        for start in range(0, len(operands), step):
            part = operands[start : start + step]
            height = part[0].shape[0]
            product = jnp.dot(
                part[0] if len(part) == 1 else jnp.concatenate(part, axis=0),
                right[t],
                preferred_element_type=f32,
            )
            for k in range(len(part)):
                yield product[k * height : (k + 1) * height]

    def density(x, y, offsets, fresh):
        t = (x - 1) * ny + y - 1
        zero = jnp.zeros((8, lanes), f32)
        rho, energy = (zero, zero) if fresh else (acc[t, 0], acc[t, 1])
        columns = [(x + a - 1, y + b - 1) for a, b in offsets]
        for (a, b), column, margin in zip(
            offsets, columns, margins([left[column] for column in columns], t)
        ):
            n = pair(x, y, a, b)
            for r in range(0, tall, 8):
                m = jnp.maximum(margin[r : r + 8], 0.0)
                u = jnp.exp2(m) * m
                q = u * spread_w[column[0], column[1], r : r + 8, :]
                rho = rho + q * m
                energy = energy + q * u
                pair_a[n, r : r + 8, :] = m
        acc[t, 0] = rho
        acc[t, 1] = energy

    def density_outer(x, y, offsets, fresh):
        t = (x - 1) * ny + y - 1
        ends = [(0, 0, slice(0, WIDE)), (slots, 2 * slots, slice(lanes - WIDE, lanes))]
        sums = [[acc[t, k, :, where] for k in range(2)] for _, _, where in ends]
        others = [(x + a - 2) * ny + y + b - 2 for a, b in offsets]
        for (a, b), other, margin in zip(
            offsets, others, margins([left_z[other] for other in others], t)
        ):
            n = pair(x, y, a, b)
            for (start, place, where), total in zip(ends, sums):
                for r in range(0, slots, 8):
                    m = jnp.maximum(margin[start + r : start + r + 8, where], 0.0)
                    u = jnp.exp2(m) * m
                    q = u * spread_z[other, start + r : start + r + 8, where]
                    total[0] = total[0] + q * m
                    total[1] = total[1] + q * u
                    rows_at = slice(place + r, place + r + 8)
                    pair_a[n, rows_at, where] = pair_a[n, rows_at, where] + m
        for (_, _, where), total in zip(ends, sums):
            for k in range(2):
                acc[t, k, :, where] = total[k]

    def twice(terms):
        return jnp.concatenate([terms, terms[:, : 2 * slots]], axis=1)

    def split(value):
        high = value.astype(bf16)
        return high, (value - high.astype(f32)).astype(bf16)

    def stack(layers):
        high, low = zip(*layers)
        return jnp.concatenate(list(high) + [low[2], low[0], low[1]], axis=0)

    def product(left_terms, values):
        return jnp.dot(twice(left_terms), values, preferred_element_type=f32)

    def force(x, y, offsets, fresh):
        t = (x - 1) * ny + y - 1
        phi = jnp.broadcast_to(phi_rows[t], (slots, lanes))
        total = None
        for a, b in offsets:
            n = pair(x, y, a, b)
            column = (x + a - 1, y + b - 1)
            layers = []
            for r in range(0, tall, slots):
                m = pair_a[n, r : r + slots, :]
                e = jnp.exp2(m)
                both = phi + spread_phi[column[0], column[1], r : r + slots, :]
                v = (e * m) * (both * (m + shift_big) + e * (m + 0.5 * shift_big))
                layers.append(split(v))
            part = product(moment[column], stack(layers))
            total = part if total is None else total + part
        acc_force[t] = total if fresh else acc_force[t] + total

    def force_fixed(x, y, offsets, fresh):
        t = (x - 1) * ny + y - 1
        phi = jnp.broadcast_to(phi_rows[t], (slots, lanes))
        total = None
        for a, b in offsets:
            n = pair(x, y, a, b)
            fixed, slope = [], []
            for r in range(0, tall, slots):
                m = pair_a[n, r : r + slots, :]
                e = jnp.exp2(m)
                u = e * m
                value = u * (m + shift_big)
                fixed.append(split(phi * value + u * (e * (m + 0.5 * shift_big))))
                slope.append(split(value))
            pair_s[n] = stack(slope)
            part = product(moment[x + a - 1, y + b - 1], stack(fixed))
            total = part if total is None else total + part
        acc_force[t] = total if fresh else acc_force[t] + total

    def force_remote(x, y, offsets, fresh):
        t = (x - 1) * ny + y - 1
        total = None
        for a, b in offsets:
            part = product(moment_phi[x + a - 1, y + b - 1], pair_s[pair(x, y, a, b)])
            total = part if total is None else total + part
        acc_force[t] = acc_force[t] + total

    def derivative_terms(x, y):
        shifted = [pad_phi[x, y, base - 1 + dz : base - 1 + dz + nz, :] for dz in (0, 1, 2, 2)]
        phi = choose(shifted)
        terms = []
        for k in range(4):
            terms += list(pieces(phi * weighted[x, y, k]))
        moment_phi[x, y] = jnp.concatenate(terms, axis=0).astype(bf16)

    def halo_columns(a, b):
        xs = range(1, nx + 1) if a == 0 else [0 if a < 0 else nx + 1]
        ys = range(1, ny + 1) if b == 0 else [0 if b < 0 else ny + 1]
        return [(x, y) for x in xs for y in ys]

    own_columns = halo_columns(0, 0)
    x_columns = halo_columns(-1, 0) + halo_columns(1, 0)
    all_halo = [
        (x, y) for x in range(nx + 2) for y in range(ny + 2) if (x, y) not in own_columns
    ]

    def around(x, y):
        return [(x + a, y + b) for a in (-1, 0, 1) for b in (-1, 0, 1)]

    far_row = jnp.where(2 * me[1] >= axis_sizes[1], 1, 0)
    near_row = 1 - far_row

    def row_of(side):
        return 1 + (ny - 1) * side, (ny + 1) * side

    def work(function, columns, fresh):
        for x, y in own_columns:
            offsets = [
                (a, b)
                for a in range(3)
                for b in range(3)
                if (x + a - 1, y + b - 1) in columns
            ]
            if offsets:
                function(x, y, offsets, fresh)

    def expand_phi(columns):
        wide = [
            choose(
                [pad_phi[x, y, base - 1 + dz : base - 1 + dz + nz, :] for dz in range(3)]
            )
            for x, y in columns
        ]
        wide = wide[0] if len(wide) == 1 else jnp.concatenate(wide, axis=1)
        stacked = jnp.concatenate(pieces(wide), axis=0).astype(bf16)
        result = lax.dot_general(
            stacked,
            hot[(used - 3) * nz : used * nz, :],
            (((0,), (0,)), ((), ())),
            preferred_element_type=f32,
        )
        for k, (x, y) in enumerate(columns):
            spread_phi[x, y] = result[k * WIDE : k * WIDE + tall]

    def start_exchange(buffer, send, recv):
        def source(step, length):
            return (
                pl.ds(length, 1) if step > 0 else pl.ds(1, 1) if step < 0 else pl.ds(1, length)
            )

        def target(step, length):
            return (
                pl.ds(0, 1)
                if step > 0
                else pl.ds(length + 1, 1) if step < 0 else pl.ds(1, length)
            )

        def source_z(step):
            return (
                pl.ds(base + nz - 1, 1)
                if step > 0
                else pl.ds(base, 1) if step < 0 else pl.ds(base, nz)
            )

        def target_z(step):
            return (
                pl.ds(base - 1, 1)
                if step > 0
                else pl.ds(base + nz, 1) if step < 0 else pl.ds(base, nz)
            )

        for direction in DIRECTIONS:
            a, b, c = direction
            pltpu.make_async_remote_copy(
                src_ref=buffer.at[source(a, nx), source(b, ny), source_z(c)],
                dst_ref=buffer.at[target(a, nx), target(b, ny), target_z(c)],
                send_sem=send,
                recv_sem=recv.at[stage(direction)],
                device_id=peer(direction),
                device_id_type=pl.DeviceIdType.MESH,
            ).start()

    def await_rows(directions, semaphore):
        count = sum(
            (1 if a else nx) * (1 if b else ny) * (1 if c else nz) for a, b, c in directions
        )
        part = blank.at[pl.ds(0, count)]
        pltpu.make_async_copy(part, part, semaphore).wait()

    def arrive(recv, number):
        kind = number if isinstance(number, int) else 2
        await_rows([d for d in DIRECTIONS if stage(d) == kind], recv.at[number])

    always = me[0] >= 0
    early = (me[0] + 1) // 2 + me[1] < 2

    def region(condition):
        return lambda function: pl.when(condition)(function)

    for x, y in own_columns:
        owner(x, y)

    def own_inner():
        for x, y in own_columns:
            neighbour(x, y, "inner")
        for x, y in own_columns:
            spread_weight(x, y, "inner")
        work(density, own_columns, True)

    region(early)(own_inner)
    pl.semaphore_wait(barrier, len(DIRECTIONS))
    start_exchange(pad, send_sem.at[0], recv_sem)
    region(jnp.logical_not(early))(own_inner)

    @region(always)
    def own_outer():
        arrive(recv_sem, 0)
        for x, y in own_columns:
            neighbour(x, y, "outer")
        for x, y in own_columns:
            spread_weight(x, y, "outer")
        work(density_outer, own_columns, False)

    def gather(value):
        total = value[:, :WIDE]
        for start in range(WIDE, lanes, WIDE):
            total = total + value[:, start : start + WIDE]
        step = WIDE // 2
        while step >= slots:
            total = total + pltpu.roll(total, step, 1)
            step //= 2
        return total

    def fold(line):
        return gather(jnp.where(cell_mask, jnp.broadcast_to(line, (nz, lanes)), 0.0))

    def halo_x():
        arrive(recv_sem, 1)
        for x, y in x_columns:
            neighbour(x, y, "all")
        for x, y in x_columns:
            spread_weight(x, y, "all")
        work(density, x_columns, False)

    def row_work(function, side):
        y = row_of(side)[0]
        for x in range(1, nx + 1):
            function(x, y, [(a, 2 * side) for a in range(3)], False)

    def halo_row(side):
        arrive(recv_sem, 3 - side)
        y = row_of(side)[1]
        for x in range(nx + 2):
            neighbour(x, y, "all")
        for x in range(nx + 2):
            spread_weight(x, y, "all")
        row_work(density, side)

    def row_columns(*sides):
        return [(x, row_of(side)[0]) for x in range(1, nx + 1) for side in sides]

    middle_columns = [(x, y) for x in range(1, nx + 1) for y in range(2, ny)]

    def derivatives(columns):
        places = [(x - 1) * ny + y - 1 for x, y in columns]
        for t in places:
            for k in range(2):
                rows[k, t] = jnp.sum(acc[t, k], axis=0, keepdims=True)
        rho, w = (jnp.concatenate([rows[k, t] for t in places], axis=0) for k in (0, 2))
        root = jnp.sqrt(jnp.maximum(rho * density_scale - w, 0.0) + 1.0)
        ratio = jnp.where(w > 1.3, 0.875, jnp.where(w > 0.5, 1.0, 0.0))
        phi = slope_scale * ratio / root
        for k, (t, (x, y)) in enumerate(zip(places, columns)):
            line = phi[k : k + 1]
            pad_phi[x, y, base : base + nz, :] = fold(line)
            phi_rows[t] = line
            rows[3, t] = root[k : k + 1]

    @region(always)
    def halo_near():
        halo_row(near_row)

    @region(always)
    def halo_sides():
        halo_x()
        derivatives(middle_columns + row_columns(near_row))

    @region(always)
    def halo_far():
        halo_row(far_row)
        derivatives(row_columns(far_row))

    start_exchange(pad_phi, send_sem.at[1], recv_phi)

    @region(always)
    def between():
        w = rows[2]
        energy = rows[1] * (energy_scale * w) - 0.25 * w * w
        a_coef = jnp.where(w > 1.3, 1.4, jnp.where(w > 0.5, 1.0, 0.0))
        rows[3] = energy - a_coef * rows[3]
        work(force_fixed, all_halo, True)

    @region(always)
    def own_force():
        arrive(recv_phi, 0)
        expand_phi(own_columns)
        for x, y in own_columns:
            inner = all(column in own_columns for column in around(x, y))
            offsets = [
                (a, b)
                for a in range(3)
                for b in range(3)
                if (x + a - 1, y + b - 1) in own_columns
            ]
            force(x, y, offsets, inner)

    def write(columns):
        for x, y in columns:
            t = (x - 1) * ny + y - 1
            sums = [
                acc_force[t, (3 * k) * nz : (3 * k + 1) * nz]
                + acc_force[t, (3 * k + 1) * nz : (3 * k + 2) * nz]
                + acc_force[t, (3 * k + 2) * nz : (3 * k + 3) * nz]
                for k in range(4)
            ]
            scale = force_scale * own[t, 3]
            lines = [gather((sums[k] - own[t, k] * sums[3]) * scale) for k in range(3)]
            out_ref[x - 1, y - 1] = choose(lines + [fold(rows[3, t])])

    def force_row(side):
        arrive(recv_phi, 3 - side)
        for x in range(nx + 2):
            derivative_terms(x, row_of(side)[1])
        row_work(force_remote, side)

    @region(always)
    def force_near():
        force_row(near_row)

    @region(always)
    def force_sides():
        arrive(recv_phi, 1)
        for x, y in x_columns:
            derivative_terms(x, y)
        work(force_remote, x_columns, False)
        write(middle_columns + row_columns(near_row))

    @region(always)
    def force_far():
        force_row(far_row)
        write(row_columns(far_row))

    for number in range(2):
        await_rows(DIRECTIONS, send_sem.at[number])


def body(axis_sizes, positions, types):
    nx, ny, nz, slots = types.shape
    lanes = nz * slots
    tall = 3 * slots
    columns = nx * ny
    deep = 16 + nz
    f32, bf16 = jnp.float32, jnp.bfloat16
    return pl.pallas_call(
        functools.partial(kernel, (nx, ny, nz, slots), axis_sizes),
        out_shape=pltpu.VMEM((nx, ny, nz, 4 * slots), f32),
        in_specs=[pl.BlockSpec(memory_space=pl.ANY), pl.BlockSpec(memory_space=pl.ANY)],
        out_specs=pl.BlockSpec(memory_space=pltpu.VMEM),
        scratch_shapes=[
            pltpu.VMEM((nx, ny, nz, 3 * slots), f32),
            pltpu.VMEM((nx, ny, nz, slots), jnp.int32),
            pltpu.VMEM((nx + 2, ny + 2, deep, WIDE), f32),
            pltpu.VMEM((nx + 2, ny + 2, deep, WIDE), f32),
            pltpu.VMEM((nx + 2, ny + 2, tall, DEEP), bf16),
            pltpu.VMEM((columns, 2 * slots, DEEP), bf16),
            pltpu.VMEM((columns, DEEP, lanes), bf16),
            pltpu.VMEM((nx + 2, ny + 2, 12 * nz, WIDE), bf16),
            pltpu.VMEM((nx + 2, ny + 2, 12 * nz, WIDE), bf16),
            pltpu.VMEM((nx + 2, ny + 2, 4, nz, WIDE), f32),
            pltpu.VMEM((nx + 2, ny + 2, tall, lanes), f32),
            pltpu.VMEM((columns, 2 * slots, lanes), f32),
            pltpu.VMEM((nx + 2, ny + 2, tall, lanes), f32),
            pltpu.VMEM((columns, 4, nz, lanes), f32),
            pltpu.VMEM((columns, 2, 8, lanes), f32),
            pltpu.VMEM((columns, 12 * nz, lanes), f32),
            pltpu.VMEM((4, columns, 1, lanes), f32),
            pltpu.VMEM((columns, 1, lanes), f32),
            pltpu.VMEM((DEEP, lanes), bf16),
            pltpu.VMEM((columns * 9, tall, lanes), f32),
            pltpu.VMEM((columns * 9, 2 * tall, lanes), bf16),
            pltpu.VMEM(((nx + 2) * (ny + 2) * nz, WIDE), f32),
            pltpu.SemaphoreType.DMA((2,)),
            pltpu.SemaphoreType.DMA((2,)),
            pltpu.SemaphoreType.DMA((4,)),
            pltpu.SemaphoreType.DMA((4,)),
        ],
        compiler_params=pltpu.CompilerParams(
            collective_id=0, has_side_effects=True, vmem_limit_bytes=60 * 1024 * 1024
        ),
    )(positions, types)


def solution(mesh):
    spec = P("gx", "gy", "gz", None)
    sizes = tuple(mesh.shape[axis] for axis in AXES)
    return jax.shard_map(
        functools.partial(body, sizes),
        mesh=mesh,
        in_specs=(spec, spec),
        out_specs=spec,
        check_vma=False,
    )
```

```python
import functools
import math

import jax
import jax.numpy as jnp
from jax import lax
from jax.experimental import pallas as pl
from jax.experimental.pallas import tpu as pltpu
from jax.sharding import PartitionSpec as P

cut_square = 0.9025
density_rate = 3.0
unit = density_rate * math.log2(math.e)
alpha = math.sqrt(unit)
kappa = unit * cut_square
tail = 2.0**-kappa
shift_big = 2.0 * kappa / (cut_square * density_rate)
density_scale = tail / kappa**2
energy_scale = 0.25 * tail**2 / kappa**2
force_scale = -2.0 * tail**2 * density_rate / (kappa**2 * alpha)
slope_scale = -0.5 / tail
far = 1.0e4

AXES = ("gx", "gy", "gz")
DIRECTIONS = sorted(
    (
        (a, b, c)
        for a in (-1, 0, 1)
        for b in (-1, 0, 1)
        for c in (-1, 0, 1)
        if (a, b, c) != (0, 0, 0)
    ),
    key=lambda d: -(2 * abs(d[0]) + 2 * abs(d[1]) + abs(d[2])),
)
def stage(direction):
    a, b, _ = direction
    return 2 + (b > 0) if b else abs(a)


WIDE = 128
DEEP = 256


def kernel(dims, axis_sizes, pos_ref, typ_ref, out_ref, pos, typ, pad, pad_phi, left, left_z, right, moment,
           moment_phi, weighted, spread_w, spread_z, spread_phi, own, acc, acc_force, rows, phi_rows, hot, pair_a, pair_b, pair_s,
           blank, load_sem, send_sem, recv_sem, recv_phi):
    nx, ny, nz, slots = dims
    lanes = nz * slots
    tall = 3 * slots
    base = 8
    f32, bf16 = jnp.float32, jnp.bfloat16
    me = [lax.axis_index(axis) for axis in AXES]

    def peer(direction):
        return {
            axis: lax.rem(place + step + size, size)
            for axis, place, step, size in zip(AXES, me, direction, axis_sizes)
        }

    barrier = pltpu.get_barrier_semaphore()
    for direction in DIRECTIONS:
        pl.semaphore_signal(
            barrier, inc=1, device_id=peer(direction), device_id_type=pl.DeviceIdType.MESH
        )
    loads = [
        pltpu.make_async_copy(pos_ref, pos, load_sem.at[0]),
        pltpu.make_async_copy(typ_ref, typ, load_sem.at[1]),
    ]
    for load in loads:
        load.start()

    cell_mask = (
        lax.broadcasted_iota(jnp.int32, (nz, lanes), 1) // slots
        == lax.broadcasted_iota(jnp.int32, (nz, lanes), 0)
    )
    cells = jnp.where(cell_mask, 1.0, 0.0).astype(f32)
    group = lax.broadcasted_iota(jnp.int32, (nz, WIDE), 1) // slots
    empty = jnp.zeros((nz, lanes), f32)
    full = jnp.ones((nz, WIDE), f32)
    none = jnp.zeros((nz, WIDE), f32)
    parts = DEEP // nz
    used = 27
    hot[...] = jnp.concatenate(
        [empty] * (used - 3) + [cells] * 3 + [empty] * (parts - used), axis=0
    ).astype(bf16)

    for load in loads:
        load.wait()
    for x in range(nx):
        for y in range(ny):
            kind = typ[x, y]
            weight = jnp.where(kind == 1, 1.0, jnp.where(kind == 2, 1.6, 0.0)).astype(f32)
            pad[x + 1, y + 1, base : base + nz, :] = jnp.concatenate(
                [pos[x, y] * alpha, weight], axis=1
            )

    def pieces(value):
        high = value.astype(bf16).astype(f32)
        rest = value - high
        middle = rest.astype(bf16).astype(f32)
        return high, middle, rest - middle

    def choose(values):
        result = values[-1]
        for k in reversed(range(len(values) - 1)):
            result = jnp.where(group == k, values[k], result)
        return result

    def turn(value, step):
        step = (step * slots) % WIDE
        return pltpu.roll(value, step, 1) if step else value

    def centre(k, place):
        return (jnp.asarray(place, f32) - (0.5 * ((nx, ny)[k] + 1) + 0.5)) * alpha

    layer = (jnp.minimum(group, 2).astype(f32) - 1.5) * alpha

    cell_row = lax.broadcasted_iota(jnp.int32, (nz, WIDE), 0)
    outside = ((group == 0) & (cell_row == 0)) | ((group == 2) & (cell_row == nz - 1))

    def neighbour(x, y, part):
        if part == "inner":
            middle = pad[x, y, base : base + nz, :]
            shifted = [
                jnp.where(cell_row == 0, 0.0, pltpu.roll(middle, 1, 0)),
                middle,
                jnp.where(cell_row == nz - 1, 0.0, pltpu.roll(middle, nz - 1, 0)),
            ]
        else:
            shifted = [pad[x, y, base - 1 + dz : base - 1 + dz + nz, :] for dz in range(3)]
        places = (0, 1, 2, 2)
        px, py, pz, w = (
            choose([turn(shifted[dz], g - q) for g, dz in enumerate(places)]) for q in range(4)
        )
        px = px + centre(0, x)
        py = py + centre(1, y)
        pz = pz + layer
        square = px * px + py * py + pz * pz
        present = w > 0.0
        if part == "outer":
            present = present & outside
        square = jnp.where(present, square, far)
        lines = []
        for value in (px, py, pz):
            h, m, l = pieces(value)
            lines += [h, m, h, l, m, h]
        lines += list(pieces(-square)) + [full] * 3
        ws = list(pieces(w))
        lines += ws + [none] * (parts - used)
        stacked = jnp.concatenate(lines, axis=0).astype(bf16).T
        if part == "outer":
            t = (x - 1) * ny + y - 1
            left_z[t, :slots] = stacked[:slots]
            left_z[t, slots:] = stacked[2 * slots : tall]
        else:
            left[x, y] = stacked[:tall]
        if part != "inner":
            values = (w * px, w * py, w * pz)
            terms = []
            for k, value in enumerate(values):
                terms += list(pieces(value))
                weighted[x, y, k] = value
            weighted[x, y, 3] = w
            moment[x, y] = jnp.concatenate(terms + ws, axis=0).astype(bf16)

    def spread_weights(columns, part):
        step = 3
        for start in range(0, len(columns), step):
            some = columns[start : start + step]
            if part == "outer":
                places = [((x - 1) * ny + y - 1,) for x, y in some]
                source, target = left_z, spread_z
            else:
                places, source, target = some, left, spread_w
            height = source.shape[-2]
            result = jnp.dot(
                jnp.concatenate([source[place] for place in places], axis=0),
                hot[...],
                preferred_element_type=f32,
            )
            for k, place in enumerate(places):
                target[place] = result[k * height : (k + 1) * height]

    def owner(x, y):
        t = (x - 1) * ny + y - 1
        value = pad[x, y, base : base + nz, :]
        px, py, pz, w = (choose([turn(value, g - q) for g in range(WIDE // slots)]) for q in range(4))
        px = px + centre(0, x)
        py = py + centre(1, y)
        pz = pz - 0.5 * alpha
        square = kappa - (px * px + py * py + pz * pz)

        def tile(value):
            return jnp.where(cell_mask, jnp.concatenate([value] * (lanes // WIDE), axis=1), 0.0)

        lines = []
        for value in (px, py, pz):
            h, m, l = (tile(2.0 * piece) for piece in pieces(value))
            lines += [h, h, m, h, m, l]
        lines += [cells] * 3 + [tile(piece) for piece in pieces(square)]
        lines += [empty] * (parts - used + 3)
        right[t] = jnp.concatenate(lines, axis=0).astype(bf16)
        for k, value in enumerate((px, py, pz, w)):
            own[t, k] = tile(value)
        rows[2, t] = jnp.sum(own[t, 3], axis=0, keepdims=True)

    def pair(x, y, a, b):
        return (((x - 1) * ny + y - 1) * 3 + a) * 3 + b

    def margins(operands, t):
        step = 3
        for start in range(0, len(operands), step):
            part = operands[start : start + step]
            height = part[0].shape[0]
            product = jnp.dot(
                part[0] if len(part) == 1 else jnp.concatenate(part, axis=0),
                right[t],
                preferred_element_type=f32,
            )
            for k in range(len(part)):
                yield product[k * height : (k + 1) * height]

    def slopes(m, e, u):
        return u * (m + shift_big), u * (e * (m + 0.5 * shift_big))

    def density(x, y, offsets, fresh):
        t = (x - 1) * ny + y - 1
        zero = jnp.zeros((8, lanes), f32)
        rho, energy = (zero, zero) if fresh else (acc[t, 0], None)
        columns = [(x + a - 1, y + b - 1) for a, b in offsets]
        for (a, b), column, margin in zip(
            offsets, columns, margins([left[column] for column in columns], t)
        ):
            n = pair(x, y, a, b)
            for r in range(0, tall, 8):
                m = jnp.maximum(margin[r : r + 8], 0.0)
                e = jnp.exp2(m)
                u = e * m
                q = u * spread_w[column[0], column[1], r : r + 8, :]
                rho = rho + q * m
                if fresh:
                    energy = energy + q * u
                    pair_a[n, r : r + 8, :], pair_b[n, r : r + 8, :] = slopes(m, e, u)
                else:
                    pair_a[n, r : r + 8, :] = m
        acc[t, 0] = rho
        if fresh:
            acc[t, 1] = energy

    def density_outer(x, y, offsets, fresh):
        t = (x - 1) * ny + y - 1
        ends = [(0, 0, slice(0, WIDE)), (slots, 2 * slots, slice(lanes - WIDE, lanes))]
        sums = [[acc[t, k, :, where] for k in range(2)] for _, _, where in ends]
        others = [(x + a - 2) * ny + y + b - 2 for a, b in offsets]
        for (a, b), other, margin in zip(
            offsets, others, margins([left_z[other] for other in others], t)
        ):
            n = pair(x, y, a, b)
            for (start, place, where), total in zip(ends, sums):
                for r in range(0, slots, 8):
                    m = jnp.maximum(margin[start + r : start + r + 8, where], 0.0)
                    e = jnp.exp2(m)
                    u = e * m
                    q = u * spread_z[other, start + r : start + r + 8, where]
                    total[0] = total[0] + q * m
                    total[1] = total[1] + q * u
                    rows_at = slice(place + r, place + r + 8)
                    slope_a, slope_b = slopes(m, e, u)
                    pair_a[n, rows_at, where] = pair_a[n, rows_at, where] + slope_a
                    pair_b[n, rows_at, where] = pair_b[n, rows_at, where] + slope_b
        for (_, _, where), total in zip(ends, sums):
            for k in range(2):
                acc[t, k, :, where] = total[k]

    def twice(terms):
        return jnp.concatenate([terms, terms[:, : 2 * slots]], axis=1)

    def split(value):
        high = value.astype(bf16)
        return high, (value - high.astype(f32)).astype(bf16)

    def stack(layers):
        high, low = zip(*layers)
        return jnp.concatenate(list(high) + [low[2], low[0], low[1]], axis=0)

    def product(left_terms, values):
        return jnp.dot(twice(left_terms), values, preferred_element_type=f32)

    def force(x, y, offsets, fresh):
        t = (x - 1) * ny + y - 1
        phi = jnp.broadcast_to(phi_rows[t], (slots, lanes))
        total = None
        for a, b in offsets:
            n = pair(x, y, a, b)
            column = (x + a - 1, y + b - 1)
            layers = []
            for r in range(0, tall, slots):
                both = phi + spread_phi[column[0], column[1], r : r + slots, :]
                v = both * pair_a[n, r : r + slots, :] + pair_b[n, r : r + slots, :]
                layers.append(split(v))
            part = product(moment[column], stack(layers))
            total = part if total is None else total + part
        acc_force[t] = total if fresh else acc_force[t] + total

    def force_fixed(x, y, offsets, fresh):
        t = (x - 1) * ny + y - 1
        phi = jnp.broadcast_to(phi_rows[t], (slots, lanes))
        total, energy = None, acc[t, 1]
        for a, b in offsets:
            n = pair(x, y, a, b)
            column = (x + a - 1, y + b - 1)
            fixed, slope = [], []
            for r in range(0, tall, slots):
                m = pair_a[n, r : r + slots, :]
                e = jnp.exp2(m)
                u = e * m
                quotas = u * u * spread_w[column[0], column[1], r : r + slots, :]
                for k in range(0, slots, 8):
                    energy = energy + quotas[k : k + 8]
                slope_a, slope_b = slopes(m, e, u)
                fixed.append(split(phi * slope_a + slope_b))
                slope.append(split(slope_a))
            pair_s[n] = stack(slope)
            part = product(moment[column], stack(fixed))
            total = part if total is None else total + part
        acc_force[t] = total if fresh else acc_force[t] + total
        acc[t, 1] = energy

    def force_remote(x, y, offsets, fresh):
        t = (x - 1) * ny + y - 1
        total = None
        for a, b in offsets:
            part = product(moment_phi[x + a - 1, y + b - 1], pair_s[pair(x, y, a, b)])
            total = part if total is None else total + part
        acc_force[t] = acc_force[t] + total

    def derivative_terms(x, y):
        shifted = [pad_phi[x, y, base - 1 + dz : base - 1 + dz + nz, :] for dz in (0, 1, 2, 2)]
        phi = choose(shifted)
        terms = []
        for k in range(4):
            terms += list(pieces(phi * weighted[x, y, k]))
        moment_phi[x, y] = jnp.concatenate(terms, axis=0).astype(bf16)

    def halo_columns(a, b):
        xs = range(1, nx + 1) if a == 0 else [0 if a < 0 else nx + 1]
        ys = range(1, ny + 1) if b == 0 else [0 if b < 0 else ny + 1]
        return [(x, y) for x in xs for y in ys]

    own_columns = halo_columns(0, 0)
    x_columns = halo_columns(-1, 0) + halo_columns(1, 0)
    all_halo = [
        (x, y) for x in range(nx + 2) for y in range(ny + 2) if (x, y) not in own_columns
    ]

    def around(x, y):
        return [(x + a, y + b) for a in (-1, 0, 1) for b in (-1, 0, 1)]

    far_row = jnp.where(2 * me[1] >= axis_sizes[1], 1, 0)
    near_row = 1 - far_row

    def row_of(side):
        return 1 + (ny - 1) * side, (ny + 1) * side

    def work(function, columns, fresh):
        for x, y in own_columns:
            offsets = [
                (a, b)
                for a in range(3)
                for b in range(3)
                if (x + a - 1, y + b - 1) in columns
            ]
            if offsets:
                function(x, y, offsets, fresh)

    def expand_phi(columns):
        wide = [
            choose(
                [pad_phi[x, y, base - 1 + dz : base - 1 + dz + nz, :] for dz in range(3)]
            )
            for x, y in columns
        ]
        wide = wide[0] if len(wide) == 1 else jnp.concatenate(wide, axis=1)
        stacked = jnp.concatenate(pieces(wide), axis=0).astype(bf16)
        result = lax.dot_general(
            stacked,
            hot[(used - 3) * nz : used * nz, :],
            (((0,), (0,)), ((), ())),
            preferred_element_type=f32,
        )
        for k, (x, y) in enumerate(columns):
            spread_phi[x, y] = result[k * WIDE : k * WIDE + tall]

    def start_exchange(buffer, send, recv):
        def source(step, length):
            return (
                pl.ds(length, 1) if step > 0 else pl.ds(1, 1) if step < 0 else pl.ds(1, length)
            )

        def target(step, length):
            return (
                pl.ds(0, 1)
                if step > 0
                else pl.ds(length + 1, 1) if step < 0 else pl.ds(1, length)
            )

        def source_z(step):
            return (
                pl.ds(base + nz - 1, 1)
                if step > 0
                else pl.ds(base, 1) if step < 0 else pl.ds(base, nz)
            )

        def target_z(step):
            return (
                pl.ds(base - 1, 1)
                if step > 0
                else pl.ds(base + nz, 1) if step < 0 else pl.ds(base, nz)
            )

        for direction in DIRECTIONS:
            a, b, c = direction
            pltpu.make_async_remote_copy(
                src_ref=buffer.at[source(a, nx), source(b, ny), source_z(c)],
                dst_ref=buffer.at[target(a, nx), target(b, ny), target_z(c)],
                send_sem=send,
                recv_sem=recv.at[stage(direction)],
                device_id=peer(direction),
                device_id_type=pl.DeviceIdType.MESH,
            ).start()

    def await_rows(directions, semaphore):
        count = sum(
            (1 if a else nx) * (1 if b else ny) * (1 if c else nz) for a, b, c in directions
        )
        part = blank.at[pl.ds(0, count)]
        pltpu.make_async_copy(part, part, semaphore).wait()

    def arrive(recv, number):
        kind = number if isinstance(number, int) else 2
        await_rows([d for d in DIRECTIONS if stage(d) == kind], recv.at[number])

    always = me[0] >= 0
    early = (me[0] + 1) // 2 + me[1] < 2

    def region(condition):
        return lambda function: pl.when(condition)(function)

    for x, y in own_columns:
        owner(x, y)

    def own_inner():
        for x, y in own_columns:
            neighbour(x, y, "inner")
        spread_weights(own_columns, "inner")
        work(density, own_columns, True)

    region(early)(own_inner)
    pl.semaphore_wait(barrier, len(DIRECTIONS))
    start_exchange(pad, send_sem.at[0], recv_sem)
    region(jnp.logical_not(early))(own_inner)

    @region(always)
    def own_outer():
        arrive(recv_sem, 0)
        for x, y in own_columns:
            neighbour(x, y, "outer")
        spread_weights(own_columns, "outer")
        work(density_outer, own_columns, False)

    def gather(value):
        total = value[:, :WIDE]
        for start in range(WIDE, lanes, WIDE):
            total = total + value[:, start : start + WIDE]
        step = WIDE // 2
        while step >= slots:
            total = total + pltpu.roll(total, step, 1)
            step //= 2
        return total

    def fold(line):
        return gather(jnp.where(cell_mask, jnp.broadcast_to(line, (nz, lanes)), 0.0))

    def halo_x():
        arrive(recv_sem, 1)
        for x, y in x_columns:
            neighbour(x, y, "all")
        spread_weights(x_columns, "all")
        work(density, x_columns, False)

    def row_work(function, side):
        y = row_of(side)[0]
        for x in range(1, nx + 1):
            function(x, y, [(a, 2 * side) for a in range(3)], False)

    def halo_row(side):
        arrive(recv_sem, 3 - side)
        y = row_of(side)[1]
        for x in range(nx + 2):
            neighbour(x, y, "all")
        spread_weights([(x, y) for x in range(nx + 2)], "all")
        row_work(density, side)

    def row_columns(*sides):
        return [(x, row_of(side)[0]) for x in range(1, nx + 1) for side in sides]

    middle_columns = [(x, y) for x in range(1, nx + 1) for y in range(2, ny)]

    def derivatives(columns):
        places = [(x - 1) * ny + y - 1 for x, y in columns]
        for t in places:
            rows[0, t] = jnp.sum(acc[t, 0], axis=0, keepdims=True)
        rho, w = (jnp.concatenate([rows[k, t] for t in places], axis=0) for k in (0, 2))
        inverse = lax.rsqrt(jnp.maximum(rho * density_scale - w, 0.0) + 1.0)
        ratio = jnp.where(w > 1.3, 0.875, jnp.where(w > 0.5, 1.0, 0.0))
        phi = slope_scale * ratio * inverse
        for k, (t, (x, y)) in enumerate(zip(places, columns)):
            line = phi[k : k + 1]
            pad_phi[x, y, base : base + nz, :] = fold(line)
            phi_rows[t] = line

    @region(always)
    def halo_near():
        halo_row(near_row)

    @region(always)
    def halo_sides():
        halo_x()
        derivatives(middle_columns + row_columns(near_row))

    @region(always)
    def halo_far():
        halo_row(far_row)
        derivatives(row_columns(far_row))

    start_exchange(pad_phi, send_sem.at[1], recv_phi)

    @region(always)
    def between():
        work(force_fixed, all_halo, True)
        for t in range(nx * ny):
            rows[1, t] = jnp.sum(acc[t, 1], axis=0, keepdims=True)
        w = rows[2]
        energy = rows[1] * (energy_scale * w) - 0.25 * w * w
        a_coef = jnp.where(w > 1.3, 1.4, jnp.where(w > 0.5, 1.0, 0.0))
        occupied = jnp.maximum(rows[0] * density_scale - w, 0.0) + 1.0
        rows[3] = energy - a_coef * jnp.sqrt(occupied)


    @region(always)
    def own_force():
        arrive(recv_phi, 0)
        expand_phi(own_columns)
        for x, y in own_columns:
            inner = all(column in own_columns for column in around(x, y))
            offsets = [
                (a, b)
                for a in range(3)
                for b in range(3)
                if (x + a - 1, y + b - 1) in own_columns
            ]
            force(x, y, offsets, inner)

    def write(columns):
        for x, y in columns:
            t = (x - 1) * ny + y - 1
            sums = [
                acc_force[t, (3 * k) * nz : (3 * k + 1) * nz]
                + acc_force[t, (3 * k + 1) * nz : (3 * k + 2) * nz]
                + acc_force[t, (3 * k + 2) * nz : (3 * k + 3) * nz]
                for k in range(4)
            ]
            scale = force_scale * own[t, 3]
            lines = [gather((sums[k] - own[t, k] * sums[3]) * scale) for k in range(3)]
            out_ref[x - 1, y - 1] = choose(lines + [fold(rows[3, t])])

    def force_row(side):
        arrive(recv_phi, 3 - side)
        for x in range(nx + 2):
            derivative_terms(x, row_of(side)[1])
        row_work(force_remote, side)

    @region(always)
    def force_near():
        force_row(near_row)

    @region(always)
    def force_sides():
        arrive(recv_phi, 1)
        for x, y in x_columns:
            derivative_terms(x, y)
        work(force_remote, x_columns, False)
        write(middle_columns + row_columns(near_row))

    @region(always)
    def force_far():
        force_row(far_row)
        write(row_columns(far_row))

    for number in range(2):
        await_rows(DIRECTIONS, send_sem.at[number])


def body(axis_sizes, positions, types):
    nx, ny, nz, slots = types.shape
    lanes = nz * slots
    tall = 3 * slots
    columns = nx * ny
    deep = 16 + nz
    f32, bf16 = jnp.float32, jnp.bfloat16
    return pl.pallas_call(
        functools.partial(kernel, (nx, ny, nz, slots), axis_sizes),
        out_shape=pltpu.VMEM((nx, ny, nz, 4 * slots), f32),
        in_specs=[pl.BlockSpec(memory_space=pl.ANY), pl.BlockSpec(memory_space=pl.ANY)],
        out_specs=pl.BlockSpec(memory_space=pltpu.VMEM),
        scratch_shapes=[
            pltpu.VMEM((nx, ny, nz, 3 * slots), f32),
            pltpu.VMEM((nx, ny, nz, slots), jnp.int32),
            pltpu.VMEM((nx + 2, ny + 2, deep, WIDE), f32),
            pltpu.VMEM((nx + 2, ny + 2, deep, WIDE), f32),
            pltpu.VMEM((nx + 2, ny + 2, tall, DEEP), bf16),
            pltpu.VMEM((columns, 2 * slots, DEEP), bf16),
            pltpu.VMEM((columns, DEEP, lanes), bf16),
            pltpu.VMEM((nx + 2, ny + 2, 12 * nz, WIDE), bf16),
            pltpu.VMEM((nx + 2, ny + 2, 12 * nz, WIDE), bf16),
            pltpu.VMEM((nx + 2, ny + 2, 4, nz, WIDE), f32),
            pltpu.VMEM((nx + 2, ny + 2, tall, lanes), f32),
            pltpu.VMEM((columns, 2 * slots, lanes), f32),
            pltpu.VMEM((nx + 2, ny + 2, tall, lanes), f32),
            pltpu.VMEM((columns, 4, nz, lanes), f32),
            pltpu.VMEM((columns, 2, 8, lanes), f32),
            pltpu.VMEM((columns, 12 * nz, lanes), f32),
            pltpu.VMEM((4, columns, 1, lanes), f32),
            pltpu.VMEM((columns, 1, lanes), f32),
            pltpu.VMEM((DEEP, lanes), bf16),
            pltpu.VMEM((columns * 9, tall, lanes), f32),
            pltpu.VMEM((columns * 9, tall, lanes), f32),
            pltpu.VMEM((columns * 9, 2 * tall, lanes), bf16),
            pltpu.VMEM(((nx + 2) * (ny + 2) * nz, WIDE), f32),
            pltpu.SemaphoreType.DMA((2,)),
            pltpu.SemaphoreType.DMA((2,)),
            pltpu.SemaphoreType.DMA((4,)),
            pltpu.SemaphoreType.DMA((4,)),
        ],
        compiler_params=pltpu.CompilerParams(
            collective_id=0, has_side_effects=True, vmem_limit_bytes=60 * 1024 * 1024
        ),
    )(positions, types)


def solution(mesh):
    spec = P("gx", "gy", "gz", None)
    sizes = tuple(mesh.shape[axis] for axis in AXES)
    return jax.shard_map(
        functools.partial(body, sizes),
        mesh=mesh,
        in_specs=(spec, spec),
        out_specs=spec,
        check_vma=False,
    )
```

```python
import functools
import math

import jax
import jax.numpy as jnp
from jax import lax
from jax.experimental import pallas as pl
from jax.experimental.pallas import tpu as pltpu
from jax.sharding import PartitionSpec as P

cut_square = 0.9025
density_rate = 3.0
unit = density_rate * math.log2(math.e)
alpha = math.sqrt(unit)
kappa = unit * cut_square
tail = 2.0**-kappa
shift_big = 2.0 * kappa / (cut_square * density_rate)
density_scale = tail / kappa**2
energy_scale = 0.25 * tail**2 / kappa**2
force_scale = -2.0 * tail**2 * density_rate / (kappa**2 * alpha)
slope_scale = -0.5 / tail
far = 1.0e4

AXES = ("gx", "gy", "gz")
DIRECTIONS = sorted(
    (
        (a, b, c)
        for a in (-1, 0, 1)
        for b in (-1, 0, 1)
        for c in (-1, 0, 1)
        if (a, b, c) != (0, 0, 0)
    ),
    key=lambda d: -(2 * abs(d[0]) + 2 * abs(d[1]) + abs(d[2])),
)
def stage(direction):
    a, b, _ = direction
    return 2 + (b > 0) if b else abs(a)


WIDE = 128
DEEP = 256


def kernel(dims, axis_sizes, pos_ref, typ_ref, out_ref, pos, typ, pad, pad_phi, left, left_z, right, moment,
           moment_phi, weighted, spread_w, spread_z, spread_phi, own, acc, acc_force, rows, phi_rows, hot, pair_a, pair_b, pair_s,
           blank, load_sem, send_sem, recv_sem, recv_phi):
    nx, ny, nz, slots = dims
    lanes = nz * slots
    tall = 3 * slots
    base = 8
    f32, bf16 = jnp.float32, jnp.bfloat16
    me = [lax.axis_index(axis) for axis in AXES]

    def peer(direction):
        return {
            axis: lax.rem(place + step + size, size)
            for axis, place, step, size in zip(AXES, me, direction, axis_sizes)
        }

    barrier = pltpu.get_barrier_semaphore()
    for direction in DIRECTIONS:
        pl.semaphore_signal(
            barrier, inc=1, device_id=peer(direction), device_id_type=pl.DeviceIdType.MESH
        )
    loads = [
        pltpu.make_async_copy(pos_ref, pos, load_sem.at[0]),
        pltpu.make_async_copy(typ_ref, typ, load_sem.at[1]),
    ]
    for load in loads:
        load.start()

    cell_mask = (
        lax.broadcasted_iota(jnp.int32, (nz, lanes), 1) // slots
        == lax.broadcasted_iota(jnp.int32, (nz, lanes), 0)
    )
    cells = jnp.where(cell_mask, 1.0, 0.0).astype(f32)
    group = lax.broadcasted_iota(jnp.int32, (nz, WIDE), 1) // slots
    empty = jnp.zeros((nz, lanes), f32)
    full = jnp.ones((nz, WIDE), f32)
    none = jnp.zeros((nz, WIDE), f32)
    parts = DEEP // nz
    used = 27
    hot[...] = jnp.concatenate(
        [empty] * (used - 3) + [cells] * 3 + [empty] * (parts - used), axis=0
    ).astype(bf16)

    for load in loads:
        load.wait()
    for x in range(nx):
        for y in range(ny):
            kind = typ[x, y]
            weight = jnp.where(kind == 1, 1.0, jnp.where(kind == 2, 1.6, 0.0)).astype(f32)
            pad[x + 1, y + 1, base : base + nz, :] = jnp.concatenate(
                [pos[x, y] * alpha, weight], axis=1
            )

    def pieces(value):
        high = value.astype(bf16).astype(f32)
        rest = value - high
        middle = rest.astype(bf16).astype(f32)
        return high, middle, rest - middle

    def choose(values):
        result = values[-1]
        for k in reversed(range(len(values) - 1)):
            result = jnp.where(group == k, values[k], result)
        return result

    def turn(value, step):
        step = (step * slots) % WIDE
        return pltpu.roll(value, step, 1) if step else value

    def centre(k, place):
        return (jnp.asarray(place, f32) - (0.5 * ((nx, ny)[k] + 1) + 0.5)) * alpha

    layer = (jnp.minimum(group, 2).astype(f32) - 1.5) * alpha

    cell_row = lax.broadcasted_iota(jnp.int32, (nz, WIDE), 0)
    outside = ((group == 0) & (cell_row == 0)) | ((group == 2) & (cell_row == nz - 1))

    def neighbour(x, y, part):
        if part == "inner":
            middle = pad[x, y, base : base + nz, :]
            shifted = [
                jnp.where(cell_row == 0, 0.0, pltpu.roll(middle, 1, 0)),
                middle,
                jnp.where(cell_row == nz - 1, 0.0, pltpu.roll(middle, nz - 1, 0)),
            ]
        else:
            shifted = [pad[x, y, base - 1 + dz : base - 1 + dz + nz, :] for dz in range(3)]
        places = (0, 1, 2, 2)
        px, py, pz, w = (
            choose([turn(shifted[dz], g - q) for g, dz in enumerate(places)]) for q in range(4)
        )
        px = px + centre(0, x)
        py = py + centre(1, y)
        pz = pz + layer
        square = px * px + py * py + pz * pz
        present = w > 0.0
        if part == "outer":
            present = present & outside
        square = jnp.where(present, square, far)
        lines = []
        for value in (px, py, pz):
            h, m, l = pieces(value)
            lines += [h, m, h, l, m, h]
        lines += list(pieces(-square)) + [full] * 3
        ws = list(pieces(w))
        lines += ws + [none] * (parts - used)
        stacked = jnp.concatenate(lines, axis=0).astype(bf16).T
        if part == "outer":
            t = (x - 1) * ny + y - 1
            left_z[t, :slots] = stacked[:slots]
            left_z[t, slots:] = stacked[2 * slots : tall]
        else:
            left[x, y] = stacked[:tall]
        if part != "inner":
            for k, value in enumerate((px, py, pz, w)):
                weighted[x, y, k] = value

    def moments(x, y):
        w = weighted[x, y, 3]
        terms = []
        for k in range(3):
            value = w * weighted[x, y, k]
            weighted[x, y, k] = value
            terms += list(pieces(value))
        moment[x, y] = jnp.concatenate(terms + list(pieces(w)), axis=0).astype(bf16)

    def spread_weights(columns, part):
        step = 3
        for start in range(0, len(columns), step):
            some = columns[start : start + step]
            if part == "outer":
                places = [((x - 1) * ny + y - 1,) for x, y in some]
                source, target = left_z, spread_z
            else:
                places, source, target = some, left, spread_w
            height = source.shape[-2]
            result = jnp.dot(
                jnp.concatenate([source[place] for place in places], axis=0),
                hot[...],
                preferred_element_type=f32,
            )
            for k, place in enumerate(places):
                target[place] = result[k * height : (k + 1) * height]

    def owner(x, y):
        t = (x - 1) * ny + y - 1
        value = pad[x, y, base : base + nz, :]
        px, py, pz, w = (choose([turn(value, g - q) for g in range(WIDE // slots)]) for q in range(4))
        px = px + centre(0, x)
        py = py + centre(1, y)
        pz = pz - 0.5 * alpha
        square = kappa - (px * px + py * py + pz * pz)

        def tile(value):
            return jnp.where(cell_mask, jnp.concatenate([value] * (lanes // WIDE), axis=1), 0.0)

        lines = []
        for value in (px, py, pz):
            h, m, l = (tile(2.0 * piece) for piece in pieces(value))
            lines += [h, h, m, h, m, l]
        lines += [cells] * 3 + [tile(piece) for piece in pieces(square)]
        lines += [empty] * (parts - used + 3)
        right[t] = jnp.concatenate(lines, axis=0).astype(bf16)
        for k, value in enumerate((px, py, pz, w)):
            own[t, k] = tile(value)
        rows[2, t] = jnp.sum(own[t, 3], axis=0, keepdims=True)

    def pair(x, y, a, b):
        return (((x - 1) * ny + y - 1) * 3 + a) * 3 + b

    def margins(operands, t):
        step = 3
        for start in range(0, len(operands), step):
            part = operands[start : start + step]
            height = part[0].shape[0]
            product = jnp.dot(
                part[0] if len(part) == 1 else jnp.concatenate(part, axis=0),
                right[t],
                preferred_element_type=f32,
            )
            for k in range(len(part)):
                yield product[k * height : (k + 1) * height]

    def slopes(m, e, u):
        return u * (m + shift_big), u * (e * (m + 0.5 * shift_big))

    def density(x, y, offsets, fresh):
        t = (x - 1) * ny + y - 1
        zero = jnp.zeros((8, lanes), f32)
        rho, energy = (zero, zero) if fresh else (acc[t, 0], None)
        columns = [(x + a - 1, y + b - 1) for a, b in offsets]
        for (a, b), column, margin in zip(
            offsets, columns, margins([left[column] for column in columns], t)
        ):
            n = pair(x, y, a, b)
            for r in range(0, tall, 8):
                m = jnp.maximum(margin[r : r + 8], 0.0)
                e = jnp.exp2(m)
                u = e * m
                q = u * spread_w[column[0], column[1], r : r + 8, :]
                rho = rho + q * m
                if fresh:
                    energy = energy + q * u
                    pair_a[n, r : r + 8, :], pair_b[n, r : r + 8, :] = slopes(m, e, u)
                else:
                    pair_a[n, r : r + 8, :] = m
        acc[t, 0] = rho
        if fresh:
            acc[t, 1] = energy

    def density_outer(x, y, offsets, fresh):
        t = (x - 1) * ny + y - 1
        ends = [(0, 0, slice(0, WIDE)), (slots, 2 * slots, slice(lanes - WIDE, lanes))]
        sums = [[acc[t, k, :, where] for k in range(2)] for _, _, where in ends]
        others = [(x + a - 2) * ny + y + b - 2 for a, b in offsets]
        for (a, b), other, margin in zip(
            offsets, others, margins([left_z[other] for other in others], t)
        ):
            n = pair(x, y, a, b)
            for (start, place, where), total in zip(ends, sums):
                for r in range(0, slots, 8):
                    m = jnp.maximum(margin[start + r : start + r + 8, where], 0.0)
                    e = jnp.exp2(m)
                    u = e * m
                    q = u * spread_z[other, start + r : start + r + 8, where]
                    total[0] = total[0] + q * m
                    total[1] = total[1] + q * u
                    rows_at = slice(place + r, place + r + 8)
                    slope_a, slope_b = slopes(m, e, u)
                    pair_a[n, rows_at, where] = pair_a[n, rows_at, where] + slope_a
                    pair_b[n, rows_at, where] = pair_b[n, rows_at, where] + slope_b
        for (_, _, where), total in zip(ends, sums):
            for k in range(2):
                acc[t, k, :, where] = total[k]

    def twice(terms):
        return jnp.concatenate([terms, terms[:, : 2 * slots]], axis=1)

    def split(value):
        high = value.astype(bf16)
        return high, (value - high.astype(f32)).astype(bf16)

    def stack(layers):
        high, low = zip(*layers)
        return jnp.concatenate(list(high) + [low[2], low[0], low[1]], axis=0)

    def product(left_terms, values):
        return jnp.dot(twice(left_terms), values, preferred_element_type=f32)

    def force(x, y, offsets, fresh):
        t = (x - 1) * ny + y - 1
        phi = jnp.broadcast_to(phi_rows[t], (slots, lanes))
        total = None
        for a, b in offsets:
            n = pair(x, y, a, b)
            column = (x + a - 1, y + b - 1)
            layers = []
            for r in range(0, tall, slots):
                both = phi + spread_phi[column[0], column[1], r : r + slots, :]
                v = both * pair_a[n, r : r + slots, :] + pair_b[n, r : r + slots, :]
                layers.append(split(v))
            part = product(moment[column], stack(layers))
            total = part if total is None else total + part
        acc_force[t] = total if fresh else acc_force[t] + total

    def force_fixed(x, y, offsets, fresh):
        t = (x - 1) * ny + y - 1
        phi = jnp.broadcast_to(phi_rows[t], (slots, lanes))
        total, energy = None, acc[t, 1]
        for a, b in offsets:
            n = pair(x, y, a, b)
            column = (x + a - 1, y + b - 1)
            fixed, slope = [], []
            for r in range(0, tall, slots):
                m = pair_a[n, r : r + slots, :]
                e = jnp.exp2(m)
                u = e * m
                quotas = u * u * spread_w[column[0], column[1], r : r + slots, :]
                for k in range(0, slots, 8):
                    energy = energy + quotas[k : k + 8]
                slope_a, slope_b = slopes(m, e, u)
                fixed.append(split(phi * slope_a + slope_b))
                slope.append(split(slope_a))
            pair_s[n] = stack(slope)
            part = product(moment[column], stack(fixed))
            total = part if total is None else total + part
        acc_force[t] = total if fresh else acc_force[t] + total
        acc[t, 1] = energy

    def force_remote(x, y, offsets, fresh):
        t = (x - 1) * ny + y - 1
        total = None
        for a, b in offsets:
            part = product(moment_phi[x + a - 1, y + b - 1], pair_s[pair(x, y, a, b)])
            total = part if total is None else total + part
        acc_force[t] = acc_force[t] + total

    def derivative_terms(x, y):
        shifted = [pad_phi[x, y, base - 1 + dz : base - 1 + dz + nz, :] for dz in (0, 1, 2, 2)]
        phi = choose(shifted)
        terms = []
        for k in range(4):
            terms += list(pieces(phi * weighted[x, y, k]))
        moment_phi[x, y] = jnp.concatenate(terms, axis=0).astype(bf16)

    def halo_columns(a, b):
        xs = range(1, nx + 1) if a == 0 else [0 if a < 0 else nx + 1]
        ys = range(1, ny + 1) if b == 0 else [0 if b < 0 else ny + 1]
        return [(x, y) for x in xs for y in ys]

    own_columns = halo_columns(0, 0)
    x_columns = halo_columns(-1, 0) + halo_columns(1, 0)
    all_halo = [
        (x, y) for x in range(nx + 2) for y in range(ny + 2) if (x, y) not in own_columns
    ]

    def around(x, y):
        return [(x + a, y + b) for a in (-1, 0, 1) for b in (-1, 0, 1)]

    far_row = jnp.where(2 * me[1] >= axis_sizes[1], 1, 0)
    near_row = 1 - far_row

    def row_of(side):
        return 1 + (ny - 1) * side, (ny + 1) * side

    def work(function, columns, fresh):
        for x, y in own_columns:
            offsets = [
                (a, b)
                for a in range(3)
                for b in range(3)
                if (x + a - 1, y + b - 1) in columns
            ]
            if offsets:
                function(x, y, offsets, fresh)

    def expand_phi(columns):
        wide = [
            choose(
                [pad_phi[x, y, base - 1 + dz : base - 1 + dz + nz, :] for dz in range(3)]
            )
            for x, y in columns
        ]
        wide = wide[0] if len(wide) == 1 else jnp.concatenate(wide, axis=1)
        stacked = jnp.concatenate(pieces(wide), axis=0).astype(bf16)
        result = lax.dot_general(
            stacked,
            hot[(used - 3) * nz : used * nz, :],
            (((0,), (0,)), ((), ())),
            preferred_element_type=f32,
        )
        for k, (x, y) in enumerate(columns):
            spread_phi[x, y] = result[k * WIDE : k * WIDE + tall]

    def start_exchange(buffer, send, recv):
        def source(step, length):
            return (
                pl.ds(length, 1) if step > 0 else pl.ds(1, 1) if step < 0 else pl.ds(1, length)
            )

        def target(step, length):
            return (
                pl.ds(0, 1)
                if step > 0
                else pl.ds(length + 1, 1) if step < 0 else pl.ds(1, length)
            )

        def source_z(step):
            return (
                pl.ds(base + nz - 1, 1)
                if step > 0
                else pl.ds(base, 1) if step < 0 else pl.ds(base, nz)
            )

        def target_z(step):
            return (
                pl.ds(base - 1, 1)
                if step > 0
                else pl.ds(base + nz, 1) if step < 0 else pl.ds(base, nz)
            )

        for direction in DIRECTIONS:
            a, b, c = direction
            pltpu.make_async_remote_copy(
                src_ref=buffer.at[source(a, nx), source(b, ny), source_z(c)],
                dst_ref=buffer.at[target(a, nx), target(b, ny), target_z(c)],
                send_sem=send,
                recv_sem=recv.at[stage(direction)],
                device_id=peer(direction),
                device_id_type=pl.DeviceIdType.MESH,
            ).start()

    def await_rows(directions, semaphore):
        count = sum(
            (1 if a else nx) * (1 if b else ny) * (1 if c else nz) for a, b, c in directions
        )
        part = blank.at[pl.ds(0, count)]
        pltpu.make_async_copy(part, part, semaphore).wait()

    def arrive(recv, number):
        kind = number if isinstance(number, int) else 2
        await_rows([d for d in DIRECTIONS if stage(d) == kind], recv.at[number])

    always = me[0] >= 0
    early = (me[0] + 1) // 2 + me[1] < 2

    def region(condition):
        return lambda function: pl.when(condition)(function)

    for x, y in own_columns:
        owner(x, y)

    def own_inner():
        for x, y in own_columns:
            neighbour(x, y, "inner")
        spread_weights(own_columns, "inner")
        work(density, own_columns, True)

    region(early)(own_inner)
    pl.semaphore_wait(barrier, len(DIRECTIONS))
    start_exchange(pad, send_sem.at[0], recv_sem)
    region(jnp.logical_not(early))(own_inner)

    @region(always)
    def own_outer():
        arrive(recv_sem, 0)
        for x, y in own_columns:
            neighbour(x, y, "outer")
        spread_weights(own_columns, "outer")
        work(density_outer, own_columns, False)

    def gather(value):
        total = value[:, :WIDE]
        for start in range(WIDE, lanes, WIDE):
            total = total + value[:, start : start + WIDE]
        step = WIDE // 2
        while step >= slots:
            total = total + pltpu.roll(total, step, 1)
            step //= 2
        return total

    def fold(line):
        return gather(jnp.where(cell_mask, jnp.broadcast_to(line, (nz, lanes)), 0.0))

    def halo_x():
        arrive(recv_sem, 1)
        for x, y in x_columns:
            neighbour(x, y, "all")
        spread_weights(x_columns, "all")
        work(density, x_columns, False)

    def row_work(function, side):
        y = row_of(side)[0]
        for x in range(1, nx + 1):
            function(x, y, [(a, 2 * side) for a in range(3)], False)

    def halo_row(side):
        arrive(recv_sem, 3 - side)
        y = row_of(side)[1]
        for x in range(nx + 2):
            neighbour(x, y, "all")
        spread_weights([(x, y) for x in range(nx + 2)], "all")
        row_work(density, side)

    def row_columns(*sides):
        return [(x, row_of(side)[0]) for x in range(1, nx + 1) for side in sides]

    middle_columns = [(x, y) for x in range(1, nx + 1) for y in range(2, ny)]

    def derivatives(columns):
        places = [(x - 1) * ny + y - 1 for x, y in columns]
        for t in places:
            rows[0, t] = jnp.sum(acc[t, 0], axis=0, keepdims=True)
        rho, w = (jnp.concatenate([rows[k, t] for t in places], axis=0) for k in (0, 2))
        inverse = lax.rsqrt(jnp.maximum(rho * density_scale - w, 0.0) + 1.0)
        ratio = jnp.where(w > 1.3, 0.875, jnp.where(w > 0.5, 1.0, 0.0))
        phi = slope_scale * ratio * inverse
        for k, (t, (x, y)) in enumerate(zip(places, columns)):
            line = phi[k : k + 1]
            pad_phi[x, y, base : base + nz, :] = fold(line)
            phi_rows[t] = line

    @region(always)
    def halo_near():
        halo_row(near_row)

    @region(always)
    def halo_sides():
        halo_x()
        derivatives(middle_columns + row_columns(near_row))

    @region(always)
    def halo_far():
        halo_row(far_row)
        derivatives(row_columns(far_row))

    start_exchange(pad_phi, send_sem.at[1], recv_phi)

    @region(always)
    def between():
        for x, y in all_halo + own_columns:
            moments(x, y)
        work(force_fixed, all_halo, True)
        for t in range(nx * ny):
            rows[1, t] = jnp.sum(acc[t, 1], axis=0, keepdims=True)
        w = rows[2]
        energy = rows[1] * (energy_scale * w) - 0.25 * w * w
        a_coef = jnp.where(w > 1.3, 1.4, jnp.where(w > 0.5, 1.0, 0.0))
        occupied = jnp.maximum(rows[0] * density_scale - w, 0.0) + 1.0
        rows[3] = energy - a_coef * jnp.sqrt(occupied)


    @region(always)
    def own_force():
        arrive(recv_phi, 0)
        expand_phi(own_columns)
        for x, y in own_columns:
            inner = all(column in own_columns for column in around(x, y))
            offsets = [
                (a, b)
                for a in range(3)
                for b in range(3)
                if (x + a - 1, y + b - 1) in own_columns
            ]
            force(x, y, offsets, inner)

    def write(columns):
        for x, y in columns:
            t = (x - 1) * ny + y - 1
            sums = [
                acc_force[t, (3 * k) * nz : (3 * k + 1) * nz]
                + acc_force[t, (3 * k + 1) * nz : (3 * k + 2) * nz]
                + acc_force[t, (3 * k + 2) * nz : (3 * k + 3) * nz]
                for k in range(4)
            ]
            scale = force_scale * own[t, 3]
            lines = [gather((sums[k] - own[t, k] * sums[3]) * scale) for k in range(3)]
            out_ref[x - 1, y - 1] = choose(lines + [fold(rows[3, t])])

    def force_row(side):
        arrive(recv_phi, 3 - side)
        for x in range(nx + 2):
            derivative_terms(x, row_of(side)[1])
        row_work(force_remote, side)

    @region(always)
    def force_near():
        force_row(near_row)

    @region(always)
    def force_sides():
        arrive(recv_phi, 1)
        for x, y in x_columns:
            derivative_terms(x, y)
        work(force_remote, x_columns, False)
        write(middle_columns + row_columns(near_row))

    @region(always)
    def force_far():
        force_row(far_row)
        write(row_columns(far_row))

    for number in range(2):
        await_rows(DIRECTIONS, send_sem.at[number])


def body(axis_sizes, positions, types):
    nx, ny, nz, slots = types.shape
    lanes = nz * slots
    tall = 3 * slots
    columns = nx * ny
    deep = 16 + nz
    f32, bf16 = jnp.float32, jnp.bfloat16
    return pl.pallas_call(
        functools.partial(kernel, (nx, ny, nz, slots), axis_sizes),
        out_shape=pltpu.VMEM((nx, ny, nz, 4 * slots), f32),
        in_specs=[pl.BlockSpec(memory_space=pl.ANY), pl.BlockSpec(memory_space=pl.ANY)],
        out_specs=pl.BlockSpec(memory_space=pltpu.VMEM),
        scratch_shapes=[
            pltpu.VMEM((nx, ny, nz, 3 * slots), f32),
            pltpu.VMEM((nx, ny, nz, slots), jnp.int32),
            pltpu.VMEM((nx + 2, ny + 2, deep, WIDE), f32),
            pltpu.VMEM((nx + 2, ny + 2, deep, WIDE), f32),
            pltpu.VMEM((nx + 2, ny + 2, tall, DEEP), bf16),
            pltpu.VMEM((columns, 2 * slots, DEEP), bf16),
            pltpu.VMEM((columns, DEEP, lanes), bf16),
            pltpu.VMEM((nx + 2, ny + 2, 12 * nz, WIDE), bf16),
            pltpu.VMEM((nx + 2, ny + 2, 12 * nz, WIDE), bf16),
            pltpu.VMEM((nx + 2, ny + 2, 4, nz, WIDE), f32),
            pltpu.VMEM((nx + 2, ny + 2, tall, lanes), f32),
            pltpu.VMEM((columns, 2 * slots, lanes), f32),
            pltpu.VMEM((nx + 2, ny + 2, tall, lanes), f32),
            pltpu.VMEM((columns, 4, nz, lanes), f32),
            pltpu.VMEM((columns, 2, 8, lanes), f32),
            pltpu.VMEM((columns, 12 * nz, lanes), f32),
            pltpu.VMEM((4, columns, 1, lanes), f32),
            pltpu.VMEM((columns, 1, lanes), f32),
            pltpu.VMEM((DEEP, lanes), bf16),
            pltpu.VMEM((columns * 9, tall, lanes), f32),
            pltpu.VMEM((columns * 9, tall, lanes), f32),
            pltpu.VMEM((columns * 9, 2 * tall, lanes), bf16),
            pltpu.VMEM(((nx + 2) * (ny + 2) * nz, WIDE), f32),
            pltpu.SemaphoreType.DMA((2,)),
            pltpu.SemaphoreType.DMA((2,)),
            pltpu.SemaphoreType.DMA((4,)),
            pltpu.SemaphoreType.DMA((4,)),
        ],
        compiler_params=pltpu.CompilerParams(
            collective_id=0, has_side_effects=True, vmem_limit_bytes=60 * 1024 * 1024
        ),
    )(positions, types)


def solution(mesh):
    spec = P("gx", "gy", "gz", None)
    sizes = tuple(mesh.shape[axis] for axis in AXES)
    return jax.shard_map(
        functools.partial(body, sizes),
        mesh=mesh,
        in_specs=(spec, spec),
        out_specs=spec,
        check_vma=False,
    )
```
